512 devices in a mesh: fsdp: 8 (over y, core), trow: 16 (over x, z_hi), tcol: 4 (over z_lo).
Axes of the slice: x: 4, y: 4, z: 16 (z_hi: 4, z_lo: 4; z = z_hi * 4 + z_lo), core: 2. Of those that a mesh axis runs over, the one named last changes fastest.
Arguments:
- tokens: bfloat16 [2048, 4096], P('fsdp', 'tcol'), may hold values from -100 to 100
- w_up: bfloat16 [4096, 16384], P('tcol', ('fsdp', 'trow')), may hold values from -0.1875 to 0.1875
- w_down: bfloat16 [16384, 4096], P(('fsdp', 'trow'), 'tcol'), may hold values from -0.046875 to 0.046875
- cotangent: bfloat16 [2048, 4096], P('fsdp', 'tcol'), may hold values from -6 to 6
Outputs:
- mixed: bfloat16 [2048, 4096], P('fsdp', 'tcol')
- input_gradient: bfloat16 [2048, 4096], P('fsdp', 'tcol')
- grad_up: bfloat16 [4096, 16384], P('tcol', ('fsdp', 'trow'))
- grad_down: bfloat16 [16384, 4096], P(('fsdp', 'trow'), 'tcol')
The draws below stay inside these ranges and needn't reach their ends.
All inputs are finite; a program needn't handle non-finite values.
Results may differ from the reference program's by a relative error of at most 0.02.
Values may be sent and summed in bfloat16 or wider, within the bound.
A program may use at most 64 MiB of HBM per device.

```python
import jax
import jax.numpy as jnp
from jax import lax

MODEL_WIDTH = 4096
FF = 16384
TOK_GRP = 256
TOKENS = 2048
N_FSDP = 8
N_TCOL = 4


def draw_tokens(key, part):
    keys = jax.random.split(jax.random.fold_in(key, 17), 3)
    rising = jnp.exp(jnp.log(3.0) * jnp.arange(MODEL_WIDTH, dtype=jnp.float32) / (MODEL_WIDTH - 1))
    column = rising * jnp.exp(jax.random.uniform(keys[1], (MODEL_WIDTH,), jnp.float32, 0.0, jnp.log(10.0))) / jnp.sqrt(30.0)
    base = jnp.clip(jax.random.normal(keys[0], (TOKENS, MODEL_WIDTH), jnp.float32), -4.0, 4.0)
    row = jnp.exp(jax.random.uniform(keys[2], (TOKENS, 1), jnp.float32, 0.0, jnp.log(10.0))) / jnp.sqrt(10.0)
    return (base * row * column[None, :]).astype(jnp.bfloat16)


def draw_w_up(key, part):
    keys = jax.random.split(jax.random.fold_in(key, 29), 2)
    position = jnp.arange(MODEL_WIDTH, dtype=jnp.float32) / (MODEL_WIDTH - 1)
    shared = jnp.clip(jax.random.normal(keys[1], (1, FF), jnp.float32), -3.0, 3.0)
    rising = jnp.exp(jnp.log(4.0) * position)
    noise = jnp.clip(jax.random.normal(keys[0], (MODEL_WIDTH, FF), jnp.float32), -4.0, 4.0)
    strength = 0.5
    rising = rising / jnp.sqrt(jnp.mean(rising * rising))
    values = rising[:, None] * (noise + strength * shared) / jnp.sqrt(1.0 * MODEL_WIDTH)
    return values.astype(jnp.bfloat16)


def shard_levels(own_key, dims, cuts, low, high):
    def one(dim, parts):
        steps = jax.random.uniform(jax.random.fold_in(jax.random.fold_in(own_key, 6), dim), (parts,), jnp.float32, low / len(cuts), high / len(cuts))
        return jnp.repeat(jnp.exp(steps), dims[dim] // parts).reshape((-1,) + (1,) * (len(dims) - dim - 1))

    level = one(*cuts[0])
    for cut in cuts[1:]:
        level = level * one(*cut)
    return level


def bell_draw(stream_key, shape, spread, reach, shards=(), kind=jnp.bfloat16):
    result = spread * jax.random.normal(stream_key, shape, jnp.float32)
    if shards:
        result = result * shard_levels(stream_key, shape, shards, -0.22, 0.18)
    return jnp.clip(result, -reach, reach).astype(kind)


def setup_inputs(seed: int = 0) -> dict:
    key_of = jax.random.split(jax.random.key(seed), 5)
    return {
        "tokens": draw_tokens(jax.random.fold_in(key_of[4], 71), 0),
        "w_up": draw_w_up(jax.random.fold_in(key_of[4], 71), 0),
        "w_down": bell_draw(key_of[2], (FF, MODEL_WIDTH), FF ** -0.5, 0.046875, ((0, 128), (1, 4))),
        "cotangent": bell_draw(key_of[3], (TOKENS, MODEL_WIDTH), 1.0, 6.0, ((0, 8), (1, 4))),
    }


def gelu_value(pre):
    phi = 0.5 * (1.0 + jax.scipy.special.erf(pre * 0.7071067811865476))
    return pre * phi

def gelu_slope(pre):
    phi = 0.5 * (1.0 + jax.scipy.special.erf(pre * 0.7071067811865476))
    return phi + pre * jnp.exp(-0.5 * pre * pre) * 0.3989422804014327

def rounded_term(value):
    low = lax.optimization_barrier(value.astype(jnp.bfloat16))
    return low.astype(jnp.float32)

def reference(tokens, w_up, w_down, cotangent):
    block = MODEL_WIDTH // N_TCOL
    input_float = tokens.astype(jnp.float32)
    token_mean = lax.optimization_barrier(jnp.sum(input_float, axis=1)) / MODEL_WIDTH
    var = lax.optimization_barrier(jnp.sum(input_float * input_float, axis=1)) / MODEL_WIDTH - token_mean * token_mean
    inverse_stddev = lax.rsqrt(var + 1e-05)
    centered_scaled = (input_float - token_mean[:, None]) * inverse_stddev[:, None]
    normalized_rows = centered_scaled.astype(jnp.bfloat16)

    def pre_step(index, total):
        start = (index * block).astype(jnp.int32)
        left = lax.dynamic_slice_in_dim(normalized_rows, start, block, 1)
        right = lax.dynamic_slice_in_dim(w_up, start, block, 0)
        return total + rounded_term(jnp.dot(left, right, preferred_element_type=jnp.float32))
    pre = lax.fori_loop(0, N_TCOL, pre_step, jnp.zeros((TOKENS, FF), jnp.float32))
    hidden = gelu_value(pre).astype(jnp.bfloat16)
    branch = jnp.dot(hidden, w_down, preferred_element_type=jnp.float32)
    mixed = (input_float + branch).astype(jnp.bfloat16)

    def down_step(index, total):
        start = (index * TOK_GRP).astype(jnp.int32)
        left = lax.dynamic_slice_in_dim(hidden, start, TOK_GRP, 0)
        right = lax.dynamic_slice_in_dim(cotangent, start, TOK_GRP, 0)
        part = lax.dot_general(left, right, (((0,), (0,)), ((), ())), preferred_element_type=jnp.float32)
        return total + rounded_term(part)
    grad_down = lax.fori_loop(0, N_FSDP, down_step, jnp.zeros((FF, MODEL_WIDTH), jnp.float32))

    def dh_step(index, total):
        start = (index * block).astype(jnp.int32)
        left = lax.dynamic_slice_in_dim(cotangent, start, block, 1)
        right = lax.dynamic_slice_in_dim(w_down, start, block, 1)
        part = lax.dot_general(left, right, (((1,), (1,)), ((), ())), preferred_element_type=jnp.float32)
        return total + rounded_term(part)
    dhid = lax.fori_loop(0, N_TCOL, dh_step, jnp.zeros((TOKENS, FF), jnp.float32))
    dpre = (dhid * gelu_slope(pre)).astype(jnp.bfloat16)

    def up_step(index, total):
        start = (index * TOK_GRP).astype(jnp.int32)
        left = lax.dynamic_slice_in_dim(normalized_rows, start, TOK_GRP, 0)
        right = lax.dynamic_slice_in_dim(dpre, start, TOK_GRP, 0)
        part = lax.dot_general(left, right, (((0,), (0,)), ((), ())), preferred_element_type=jnp.float32)
        return total + rounded_term(part)
    grad_up = lax.fori_loop(0, N_FSDP, up_step, jnp.zeros((MODEL_WIDTH, FF), jnp.float32))
    normed_gradient = lax.dot_general(dpre, w_up, (((1,), (1,)), ((), ())), preferred_element_type=jnp.float32)
    first_moment = lax.optimization_barrier(jnp.sum(normed_gradient, axis=1)) / MODEL_WIDTH
    second_moment = lax.optimization_barrier(jnp.sum(normed_gradient * centered_scaled, axis=1)) / MODEL_WIDTH
    input_gradient = cotangent.astype(jnp.float32) + inverse_stddev[:, None] * (normed_gradient - first_moment[:, None] - centered_scaled * second_moment[:, None])
    return (mixed, input_gradient.astype(jnp.bfloat16), grad_up.astype(jnp.bfloat16), grad_down.astype(jnp.bfloat16))
```

```python
import jax
import jax.numpy as jnp
from jax import lax
from jax.experimental import pallas as pl
from jax.experimental.pallas import tpu as pltpu
from jax.sharding import PartitionSpec as P

BF = jnp.bfloat16
F32 = jnp.float32
OWN, PREV, NEXT, FAR = 0, 1, 2, 3


def gelu_value(pre):
    phi = 0.5 * (1.0 + lax.erf(pre * 0.7071067811865476))
    return pre * phi


def gelu_slope(pre):
    phi = 0.5 * (1.0 + lax.erf(pre * 0.7071067811865476))
    return phi + pre * jnp.exp(-0.5 * pre * pre) * 0.3989422804014327


def dot(left, right, left_dim, right_dim):
    return lax.dot_general(
        left, right, (((left_dim,), (right_dim,)), ((), ())), preferred_element_type=F32
    )


class Wire:
    def __init__(self, send_sems, recv_sems):
        self.send_sems, self.recv_sems = send_sems, recv_sems
        self.count = 0
        self.sent = []

    def slot(self):
        self.count += 1
        return self.count - 1

    def copy(self, src, dst, device, slot):
        return pltpu.make_async_remote_copy(
            src_ref=src,
            dst_ref=dst,
            send_sem=self.send_sems.at[slot],
            recv_sem=self.recv_sems.at[slot],
            device_id=device,
            device_id_type=pl.DeviceIdType.MESH,
        )

    def send(self, src, dst, device, slot=None, when=None):
        slot = self.slot() if slot is None else slot
        made = self.copy(src, dst, device, slot)
        if when is None:
            made.start()
        else:
            pl.when(when)(made.start)
        self.sent.append((made, when))
        return made

    def drain(self):
        for made, when in self.sent:
            if when is None:
                made.wait_send()
            else:
                pl.when(when)(made.wait_send)


class RingSum:
    def __init__(self, wire, plus, minus, block, half, bufs):
        self.w, self.plus, self.minus, self.block, self.half = wire, plus, minus, block, half
        self.r1a, self.r1b, self.r2p, self.r2m, self.ga, self.gb = bufs

    def start(self):
        w, half = self.w, self.half
        self.c1 = w.send(self.block(2, 0), self.r1a, self.plus)
        self.c2 = w.send(self.block(2, 1), self.r1b, self.minus)
        self.c3 = w.send(self.block(1, 1), half(self.r2p, 1), self.plus)
        self.c4 = w.send(self.block(-1, 0), half(self.r2m, 0), self.minus)

    def mid(self):
        w, half = self.w, self.half
        self.c1.wait_recv()
        self.ga[...] = (self.block(1, 0)[...].astype(F32) + self.r1a[...].astype(F32)).astype(BF)
        self.c5 = w.send(self.ga, half(self.r2p, 0), self.plus)
        self.c2.wait_recv()
        self.gb[...] = (self.block(-1, 1)[...].astype(F32) + self.r1b[...].astype(F32)).astype(BF)
        self.c6 = w.send(self.gb, half(self.r2m, 1), self.minus)

    def end(self, own):
        for c in (self.c3, self.c4, self.c5, self.c6):
            c.wait_recv()
        return own + self.r2p[...].astype(F32) + self.r2m[...].astype(F32)


class RingCopy:
    def __init__(self, wire, plus, minus, own, at_plus, at_minus, near, far):
        self.w, self.plus, self.minus = wire, plus, minus
        self.own, self.at_plus, self.at_minus, self.near, self.far = own, at_plus, at_minus, near, far

    def start(self):
        w = self.w
        self.p0 = w.send(self.own(0), self.at_plus(0), self.plus)
        self.m1 = w.send(self.own(1), self.at_minus(1), self.minus)
        self.p1 = w.send(self.own(1), self.at_plus(1), self.plus)
        self.m0 = w.send(self.own(0), self.at_minus(0), self.minus)

    def mid(self):
        w = self.w
        self.p0.wait_recv()
        self.f0 = w.send(self.near(-1, 0), self.far(-1, 0), self.plus)
        self.m1.wait_recv()
        self.f1 = w.send(self.near(1, 1), self.far(1, 1), self.minus)

    def near_end(self):
        self.p1.wait_recv()
        self.m0.wait_recv()

    def far_end(self):
        self.f0.wait_recv()
        self.f1.wait_recv()


SCRATCH = dict(
    x=((512, 1024), BF),
    c=((512, 1024), BF),
    tk=((256, 1024), BF),
    wu=((1024, 512), BF),
    wd=((512, 1024), BF),
    sstat=((8, 256), F32),
    rstat=((3, 8, 256), F32),
    mean=((256, 128), F32),
    rstd=((256, 128), F32),
    part=((2, 512, 512), BF),
    pa=((2, 4, 128, 128), BF),
    pf=((2, 4, 128, 128), BF),
    pb=((2, 4, 2, 128, 128), BF),
    pg=((2, 4, 2, 128, 128), BF),
    pre=((128, 512), F32),
    hid=((2, 512, 512), BF),
    bs=((2, 256, 1024), BF),
    br=((2, 256, 1024), BF),
    xacc=((2, 256, 1024), F32),
    xs=((2, 256, 1024), BF),
    x1a=((2, 64, 512), BF),
    x1b=((2, 64, 512), BF),
    x2p=((2, 64, 1024), BF),
    x2m=((2, 64, 1024), BF),
    xga=((2, 64, 512), BF),
    xgb=((2, 64, 512), BF),
    zacc=((2, 64, 1024), F32),
    zs=((2, 64, 1024), BF),
    z1a=((2, 16, 512), BF),
    z1b=((2, 16, 512), BF),
    z2p=((2, 16, 1024), BF),
    z2m=((2, 16, 1024), BF),
    zga=((2, 16, 512), BF),
    zgb=((2, 16, 512), BF),
    fin=((2, 256, 1024), BF),
    ts=((16, 128), F32),
    tr=((3, 16, 128), F32),
    gdp=((512, 1024), BF),
    gdo=((128, 1024), F32),
    gd1a=((64, 1024), BF),
    gd1b=((64, 1024), BF),
    gd2p=((128, 1024), BF),
    gd2m=((128, 1024), BF),
    gdga=((64, 1024), BF),
    gdgb=((64, 1024), BF),
    gdout=((128, 1024), BF),
    gup=((1024, 512), BF),
    guo=((1024, 128), F32),
    gu1a=((512, 128), BF),
    gu1b=((512, 128), BF),
    gu2p=((1024, 128), BF),
    gu2m=((1024, 128), BF),
    guga=((512, 128), BF),
    gugb=((512, 128), BF),
    guout=((1024, 128), BF),
)
N_SEMS = 176


def rows_of(index, size):
    return pl.ds(pl.multiple_of(index * size, size), size)


def kernel(tok_h, wu_h, wd_h, cot_h, mix_h, ing_h, gu_h, gd_h, *scratch):
    s = dict(zip(SCRATCH, scratch))
    send_sems, recv_sems, local_sems = scratch[len(SCRATCH) :]
    wire = Wire(send_sems, recv_sems)

    fsdp, trow, tcol = lax.axis_index("fsdp"), lax.axis_index("trow"), lax.axis_index("tcol")
    y, core = fsdp // 2, lax.rem(fsdp, 2)
    xx, zh = trow // 4, lax.rem(trow, 4)
    zl = tcol

    def at(dy=0, dcore=0, dx=0, dzh=0):
        return (
            lax.rem(y + dy, 4) * 2 + lax.rem(core + dcore, 2),
            lax.rem(xx + dx, 4) * 4 + lax.rem(zh + dzh, 4),
            tcol,
        )

    def at_zl(index):
        return (fsdp, trow, index)

    partner = at(dcore=1)
    y_plus, y_minus = at(dy=1), at(dy=3)
    x_plus, x_minus = at(dx=1), at(dx=3)
    z_plus, z_minus = at(dzh=1), at(dzh=3)
    right = zl // 2
    mate = zl + 1 - 2 * lax.rem(zl, 2)
    far_hub = 2 - right
    far_end = 3 - 3 * right
    is_hub = jnp.logical_or(zl == 1, zl == 2)
    is_end = jnp.logical_or(zl == 0, zl == 3)

    barrier = pltpu.get_barrier_semaphore()
    others = [partner, y_plus, y_minus, x_plus, x_minus, z_plus, z_minus]
    others += [at_zl(lax.rem(zl + k, 4)) for k in (1, 2, 3)]
    loads = [
        pltpu.make_async_copy(src, dst, local_sems.at[i])
        for i, (src, dst) in enumerate(
            (
                (tok_h, s["tk"]),
                (wu_h, s["wu"].at[:, 0:128]),
                (wd_h, s["wd"].at[0:128]),
                (cot_h, s["c"].at[0:256]),
            )
        )
    ]
    for load in loads:
        load.start()
    for other in others:
        pl.semaphore_signal(
            barrier, inc=1, device_id=other, device_id_type=pl.DeviceIdType.MESH
        )

    loads[0].wait()
    tok = s["tk"][...].astype(F32)
    sum_one = jnp.sum(tok, axis=1, keepdims=True)
    sum_two = jnp.sum(tok * tok, axis=1, keepdims=True)
    lane = lax.broadcasted_iota(jnp.int32, (256, 128), 1)
    both = jnp.where(lane == 0, sum_one, jnp.where(lane == 1, sum_two, 0.0))
    s["sstat"][...] = jnp.transpose(both)[0:8]
    for load in loads[1:]:
        load.wait()
    pl.semaphore_wait(barrier, len(others))

    def wu_at(pos, h):
        return s["wu"].at[h * 512 : (h + 1) * 512, pos * 128 : (pos + 1) * 128]

    def wd_at(pos, h):
        return s["wd"].at[pos * 128 + h * 64 : pos * 128 + (h + 1) * 64]

    def weights(view):
        return RingCopy(
            wire,
            y_plus,
            y_minus,
            own=lambda h: view(OWN, h),
            at_plus=lambda h: view(PREV, h),
            at_minus=lambda h: view(NEXT, h),
            near=lambda rel, h: view(PREV if rel < 0 else NEXT, h),
            far=lambda rel, h: view(FAR, h),
        )

    ups, downs = weights(wu_at), weights(wd_at)
    ups.start()
    stat_copies = [
        wire.send(s["sstat"], s["rstat"].at[k - 1], at_zl(lax.rem(zl + k, 4))) for k in (1, 2, 3)
    ]
    cot_copy = wire.send(s["c"].at[0:256], s["c"].at[256:512], partner)

    class Exchange:
        def __init__(self, which, pos):
            self.which, self.pos = which, pos
            self.lanes = slice(pos * 128, (pos + 1) * 128)

        def quarter(self, index):
            return s["part"].at[self.which, rows_of(index, 128), self.lanes]

        def start(self):
            i = (self.which, self.pos)
            b0, b1 = wire.slot(), wire.slot()
            self.b0 = wire.send(
                self.quarter(far_end), s["pb"].at[i + (1,)], at_zl(mate), b0, is_end
            )
            self.b1 = wire.send(
                self.quarter(far_hub), s["pb"].at[i + (0,)], at_zl(mate), b1, is_end
            )
            self.a = wire.send(self.quarter(mate), s["pa"].at[i], at_zl(mate))

        def mid(self):
            i = (self.which, self.pos)
            f = wire.slot()
            made_h = wire.copy(s["pg"].at[i + (0,)], s["pf"].at[i], at_zl(far_hub), f)
            g = wire.slot()
            made_e = pltpu.make_async_remote_copy(
                src_ref=s["pg"].at[i + (1,)],
                dst_ref=s["pf"].at[i],
                send_sem=send_sems.at[g],
                recv_sem=recv_sems.at[f],
                device_id=at_zl(far_end),
                device_id_type=pl.DeviceIdType.MESH,
            )

            @pl.when(is_hub)
            def _():
                self.b0.wait_recv()
                end_sum = self.quarter(far_end)[...].astype(F32) + s["pb"][i + (1,)].astype(F32)
                s["pg"][i + (1,)] = end_sum.astype(BF)
                made_e.start()
                self.b1.wait_recv()
                hub_sum = self.quarter(far_hub)[...].astype(F32) + s["pb"][i + (0,)].astype(F32)
                s["pg"][i + (0,)] = hub_sum.astype(BF)
                made_h.start()

            wire.sent.append((made_h, is_hub))
            wire.sent.append((made_e, is_hub))
            self.f = made_h

        def end(self):
            i = (self.which, self.pos)
            self.a.wait_recv()
            self.f.wait_recv()
            own = self.quarter(zl)[...].astype(F32)
            return own + s["pa"][i].astype(F32) + s["pf"][i].astype(F32)

        def back_view(self, index):
            return s["hid"].at[self.which, rows_of(index, 128), self.lanes]

        def back_start(self, value):
            s["hid"][self.which, rows_of(zl, 128), self.lanes] = value
            mine = self.back_view(zl)
            self.to_mate = wire.send(mine, mine, at_zl(mate))
            f1, f2 = wire.slot(), wire.slot()
            self.hub_slot, self.end_slot = f1, f2
            self.from_hub = wire.send(mine, mine, at_zl(far_hub), f1, is_hub)
            self.from_end = wire.send(mine, mine, at_zl(far_hub), f2, is_end)

        def back_mid(self):
            a, b = self.back_view(far_hub), self.back_view(far_end)
            g1, g2 = wire.slot(), wire.slot()
            made = []
            for ref, g, f in ((a, g1, self.hub_slot), (b, g2, self.end_slot)):
                made.append(
                    pltpu.make_async_remote_copy(
                        src_ref=ref,
                        dst_ref=ref,
                        send_sem=send_sems.at[g],
                        recv_sem=recv_sems.at[f],
                        device_id=at_zl(mate),
                        device_id_type=pl.DeviceIdType.MESH,
                    )
                )

            @pl.when(is_hub)
            def _():
                self.from_hub.wait_recv()
                made[0].start()
                self.from_end.wait_recv()
                made[1].start()

            wire.sent += [(made[0], is_hub), (made[1], is_hub)]

        def back_end(self):
            self.to_mate.wait_recv()

            @pl.when(is_end)
            def _():
                self.from_hub.wait_recv()
                self.from_end.wait_recv()

    pres = [Exchange(0, pos) for pos in range(4)]
    dhs = [Exchange(1, pos) for pos in range(4)]

    def pre_part(first, last):
        lanes = slice(first * 128, last * 128)
        s["part"][0, :, lanes] = dot(s["x"][...], s["wu"][:, lanes], 1, 0).astype(BF)
        for pos in range(first, last):
            pres[pos].start()

    def dh_part(first, last):
        lanes = slice(first * 128, last * 128)
        s["part"][1, :, lanes] = dot(s["c"][...], s["wd"][lanes], 1, 1).astype(BF)
        for pos in range(first, last):
            dhs[pos].start()

    def pre_done(pos):
        lanes = slice(pos * 128, (pos + 1) * 128)
        pre = pres[pos].end()
        s["pre"][:, lanes] = pre
        pres[pos].back_start(gelu_value(pre).astype(BF))

    def dh_done(pos):
        lanes = slice(pos * 128, (pos + 1) * 128)
        dhs[pos].back_start((dhs[pos].end() * gelu_slope(s["pre"][:, lanes])).astype(BF))

    cot_copy.wait_recv()
    dh_part(0, 1)

    for c in stat_copies:
        c.wait_recv()
    total = s["sstat"][...] + s["rstat"][0] + s["rstat"][1] + s["rstat"][2]
    total = jnp.transpose(jnp.concatenate([total, jnp.zeros((120, 256), F32)], axis=0))
    mean = total[:, 0:1] / 4096.0
    var = total[:, 1:2] / 4096.0 - mean * mean
    rstd = lax.rsqrt(var + 1e-05)
    s["mean"][...] = jnp.broadcast_to(mean, (256, 128))
    s["rstd"][...] = jnp.broadcast_to(rstd, (256, 128))
    s["x"][0:256] = ((s["tk"][...].astype(F32) - mean) * rstd).astype(BF)
    x_copy = wire.send(s["x"].at[0:256], s["x"].at[256:512], partner)
    ups.mid()
    downs.start()
    x_copy.wait_recv()
    pre_part(0, 1)
    dhs[0].mid()
    ups.near_end()
    pre_part(1, 3)
    pres[0].mid()
    ups.far_end()
    pre_part(3, 4)
    pre_done(0)
    dh_done(0)
    pres[1].mid()
    pres[2].mid()
    downs.mid()
    pres[0].back_mid()
    dhs[0].back_mid()
    pres[3].mid()
    pre_done(1)
    pre_done(2)
    pre_done(3)
    downs.near_end()
    dh_part(1, 3)
    for pos in (1, 2, 3):
        pres[pos].back_mid()
    dhs[1].mid()
    dhs[2].mid()
    downs.far_end()
    dh_part(3, 4)

    def out_part(o, product):
        s["bs"][o] = product[256:512].astype(BF)
        s["xacc"][o] = product[0:256]
        return wire.send(s["bs"].at[o], s["br"].at[o], partner)

    def over_x(o):
        def block(rel, h):
            return s["xs"].at[o, rows_of(lax.rem(xx + rel + 4, 4), 64), h * 512 : (h + 1) * 512]

        def half(ref, h):
            return ref.at[:, h * 512 : (h + 1) * 512]

        names = ("x1a", "x1b", "x2p", "x2m", "xga", "xgb")
        return RingSum(wire, x_plus, x_minus, block, half, [s[n].at[o] for n in names])

    def over_z(o):
        def block(rel, h):
            return s["zs"].at[o, rows_of(lax.rem(zh + rel + 4, 4), 16), h * 512 : (h + 1) * 512]

        def half(ref, h):
            return ref.at[:, h * 512 : (h + 1) * 512]

        names = ("z1a", "z1b", "z2p", "z2m", "zga", "zgb")
        return RingSum(wire, z_plus, z_minus, block, half, [s[n].at[o] for n in names])

    x_sums, z_sums = [over_x(0), over_x(1)], [over_z(0), over_z(1)]

    def x_start(o, copy):
        copy.wait_recv()
        value = s["xacc"][o] + s["br"][o].astype(F32)
        s["xacc"][o] = value
        s["xs"][o] = value.astype(BF)
        x_sums[o].start()

    def z_start(o):
        value = x_sums[o].end(s["xacc"][o, rows_of(xx, 64)])
        s["zacc"][o] = value
        s["zs"][o] = value.astype(BF)
        z_sums[o].start()

    def z_done(o):
        return z_sums[o].end(s["zacc"][o, rows_of(zh, 16)])

    def spread(o, index_of, size, plus, minus):
        def view(rel, h):
            return s["fin"].at[o, index_of(rel, size), h * 512 : (h + 1) * 512]

        return RingCopy(
            wire,
            plus,
            minus,
            own=lambda h: view(0, h),
            at_plus=lambda h: view(0, h),
            at_minus=lambda h: view(0, h),
            near=view,
            far=view,
        )

    def z_rows(rel, size):
        return pl.ds(pl.multiple_of(xx * 64 + lax.rem(zh + rel + 4, 4) * 16, 16), 16)

    def x_rows(rel, size):
        return rows_of(lax.rem(xx + rel + 4, 4), 64)

    z_spreads = [spread(o, z_rows, 16, z_plus, z_minus) for o in (0, 1)]
    x_spreads = [spread(o, x_rows, 64, x_plus, x_minus) for o in (0, 1)]

    pos_of = {1: NEXT, 2: FAR, -1: PREV}

    def gd_block(rel, h):
        first = pos_of[rel] * 128 + h * 64
        return s["gdp"].at[first : first + 64]

    def gu_block(rel, h):
        pos = pos_of[rel]
        return s["gup"].at[h * 512 : (h + 1) * 512, pos * 128 : (pos + 1) * 128]

    gd_names = ("gd1a", "gd1b", "gd2p", "gd2m", "gdga", "gdgb")
    gu_names = ("gu1a", "gu1b", "gu2p", "gu2m", "guga", "gugb")
    gd_sum = RingSum(
        wire, y_plus, y_minus, gd_block, lambda r, h: r.at[h * 64 : (h + 1) * 64],
        [s[n] for n in gd_names],
    )
    gu_sum = RingSum(
        wire, y_plus, y_minus, gu_block, lambda r, h: r.at[h * 512 : (h + 1) * 512],
        [s[n] for n in gu_names],
    )

    for pos in range(4):
        pres[pos].back_end()
    branch_copy = out_part(0, dot(s["hid"][0], s["wd"][...], 1, 0))
    dh_done(1)
    dh_done(2)
    dhs[3].mid()
    x_start(0, branch_copy)
    grad = dot(s["hid"][0], s["c"][...], 0, 0)
    s["gdo"][...] = grad[0:128]
    s["gdp"][128:512] = grad[128:512].astype(BF)
    gd_sum.start()
    dhs[1].back_mid()
    dhs[2].back_mid()
    dh_done(3)
    x_sums[0].mid()
    dhs[3].back_mid()
    for pos in range(4):
        dhs[pos].back_end()

    dnorm_copy = out_part(1, dot(s["hid"][1], s["wu"][...], 1, 1))
    z_start(0)
    x_start(1, dnorm_copy)
    gd_sum.mid()
    grad = dot(s["x"][...], s["hid"][1], 0, 0)
    s["guo"][...] = grad[:, 0:128]
    s["gup"][:, 128:512] = grad[:, 128:512].astype(BF)
    gu_sum.start()
    z_sums[0].mid()
    x_sums[1].mid()

    mine = z_rows(0, 16)
    tok_mine = s["tk"][mine, :].astype(F32)
    z_start(1)
    s["fin"][0, mine, :] = (tok_mine + z_done(0)).astype(BF)
    z_spreads[0].start()
    gu_sum.mid()
    z_sums[1].mid()
    s["gdout"][...] = gd_sum.end(s["gdo"][...]).astype(BF)
    gd_out = pltpu.make_async_copy(s["gdout"], gd_h, local_sems.at[4])
    gd_out.start()
    z_spreads[0].mid()

    dnorm = z_done(1)
    xhat = (tok_mine - s["mean"][mine, 0:1]) * s["rstd"][mine, 0:1]
    first = jnp.sum(dnorm, axis=1, keepdims=True)
    second = jnp.sum(dnorm * xhat, axis=1, keepdims=True)
    lane = lax.broadcasted_iota(jnp.int32, (16, 128), 1)
    s["ts"][...] = jnp.where(lane == 0, first, jnp.where(lane == 1, second, 0.0))
    moment_copies = [
        wire.send(s["ts"], s["tr"].at[k - 1], at_zl(lax.rem(zl + k, 4))) for k in (1, 2, 3)
    ]
    z_spreads[0].near_end()
    z_spreads[0].far_end()
    x_spreads[0].start()
    for c in moment_copies:
        c.wait_recv()
    moments = s["ts"][...] + s["tr"][0] + s["tr"][1] + s["tr"][2]
    moments = moments / 4096.0
    cot_mine = s["c"][mine, :].astype(F32)
    grad = cot_mine + s["rstd"][mine, 0:1] * (dnorm - moments[:, 0:1] - xhat * moments[:, 1:2])
    s["fin"][1, mine, :] = grad.astype(BF)
    z_spreads[1].start()
    x_spreads[0].mid()
    s["guout"][...] = gu_sum.end(s["guo"][...]).astype(BF)
    gu_out = pltpu.make_async_copy(s["guout"], gu_h, local_sems.at[5])
    gu_out.start()
    z_spreads[1].mid()
    x_spreads[0].near_end()
    x_spreads[0].far_end()
    mix_out = pltpu.make_async_copy(s["fin"].at[0], mix_h, local_sems.at[6])
    mix_out.start()
    z_spreads[1].near_end()
    z_spreads[1].far_end()
    x_spreads[1].start()
    x_spreads[1].mid()
    x_spreads[1].near_end()
    x_spreads[1].far_end()
    ing_out = pltpu.make_async_copy(s["fin"].at[1], ing_h, local_sems.at[7])
    ing_out.start()
    wire.drain()
    assert wire.count <= N_SEMS, wire.count
    for out in (gd_out, gu_out, mix_out, ing_out):
        out.wait()


def local(tokens, w_up, w_down, cotangent):
    scratch = [pltpu.VMEM(shape, dtype) for shape, dtype in SCRATCH.values()]
    scratch += [pltpu.SemaphoreType.DMA((N_SEMS,)), pltpu.SemaphoreType.DMA((N_SEMS,))]
    scratch += [pltpu.SemaphoreType.DMA((8,))]
    return pl.pallas_call(
        kernel,
        out_shape=(
            jax.ShapeDtypeStruct(tokens.shape, BF),
            jax.ShapeDtypeStruct(cotangent.shape, BF),
            jax.ShapeDtypeStruct(w_up.shape, BF),
            jax.ShapeDtypeStruct(w_down.shape, BF),
        ),
        in_specs=[pl.BlockSpec(memory_space=pl.ANY)] * 4,
        out_specs=[pl.BlockSpec(memory_space=pl.ANY)] * 4,
        scratch_shapes=scratch,
        compiler_params=pltpu.CompilerParams(
            collective_id=0, has_side_effects=True, vmem_limit_bytes=60000 * 1024
        ),
        name="block",
    )(tokens, w_up, w_down, cotangent)


def solution(mesh):
    return jax.shard_map(
        local,
        mesh=mesh,
        in_specs=(
            P("fsdp", "tcol"),
            P("tcol", ("fsdp", "trow")),
            P(("fsdp", "trow"), "tcol"),
            P("fsdp", "tcol"),
        ),
        out_specs=(
            P("fsdp", "tcol"),
            P("fsdp", "tcol"),
            P("tcol", ("fsdp", "trow")),
            P(("fsdp", "trow"), "tcol"),
        ),
        check_vma=False,
    )
```

```python
import jax
import jax.numpy as jnp
from jax import lax
from jax.experimental import pallas as pl
from jax.experimental.pallas import tpu as pltpu
from jax.sharding import PartitionSpec as P

BF = jnp.bfloat16
F32 = jnp.float32
OWN, PREV, NEXT, FAR = 0, 1, 2, 3


def gelu_value(pre):
    phi = 0.5 * (1.0 + lax.erf(pre * 0.7071067811865476))
    return pre * phi


def gelu_slope(pre):
    phi = 0.5 * (1.0 + lax.erf(pre * 0.7071067811865476))
    return phi + pre * jnp.exp(-0.5 * pre * pre) * 0.3989422804014327


def dot(left, right, left_dim, right_dim):
    return lax.dot_general(
        left, right, (((left_dim,), (right_dim,)), ((), ())), preferred_element_type=F32
    )


class Wire:
    def __init__(self, send_sems, recv_sems):
        self.send_sems, self.recv_sems = send_sems, recv_sems
        self.count = 0
        self.sent = []

    def slot(self):
        self.count += 1
        return self.count - 1

    def copy(self, src, dst, device, slot):
        return pltpu.make_async_remote_copy(
            src_ref=src,
            dst_ref=dst,
            send_sem=self.send_sems.at[slot],
            recv_sem=self.recv_sems.at[slot],
            device_id=device,
            device_id_type=pl.DeviceIdType.MESH,
        )

    def send(self, src, dst, device, slot=None, when=None):
        slot = self.slot() if slot is None else slot
        made = self.copy(src, dst, device, slot)
        if when is None:
            made.start()
        else:
            pl.when(when)(made.start)
        self.sent.append((made, when))
        return made

    def drain(self):
        for made, when in self.sent:
            if when is None:
                made.wait_send()
            else:
                pl.when(when)(made.wait_send)


class RingSum:
    def __init__(self, wire, plus, minus, block, half, bufs):
        self.w, self.plus, self.minus, self.block, self.half = wire, plus, minus, block, half
        self.r1a, self.r1b, self.r2p, self.r2m, self.ga, self.gb = bufs

    def start(self):
        self.start_far()
        self.start_near()

    def start_far(self):
        w = self.w
        self.c1 = w.send(self.block(2, 0), self.r1a, self.plus)
        self.c2 = w.send(self.block(2, 1), self.r1b, self.minus)

    def start_near(self):
        w, half = self.w, self.half
        self.c3 = w.send(self.block(1, 1), half(self.r2p, 1), self.plus)
        self.c4 = w.send(self.block(-1, 0), half(self.r2m, 0), self.minus)

    def mid(self):
        w, half = self.w, self.half
        self.c1.wait_recv()
        self.ga[...] = (self.block(1, 0)[...].astype(F32) + self.r1a[...].astype(F32)).astype(BF)
        self.c5 = w.send(self.ga, half(self.r2p, 0), self.plus)
        self.c2.wait_recv()
        self.gb[...] = (self.block(-1, 1)[...].astype(F32) + self.r1b[...].astype(F32)).astype(BF)
        self.c6 = w.send(self.gb, half(self.r2m, 1), self.minus)

    def end(self, own):
        for c in (self.c3, self.c4, self.c5, self.c6):
            c.wait_recv()
        return own + self.r2p[...].astype(F32) + self.r2m[...].astype(F32)


class RingCopy:
    def __init__(self, wire, plus, minus, own, at_plus, at_minus, near, far):
        self.w, self.plus, self.minus = wire, plus, minus
        self.own, self.at_plus, self.at_minus, self.near, self.far = own, at_plus, at_minus, near, far

    def start(self):
        w = self.w
        self.p0 = w.send(self.own(0), self.at_plus(0), self.plus)
        self.m1 = w.send(self.own(1), self.at_minus(1), self.minus)
        self.p1 = w.send(self.own(1), self.at_plus(1), self.plus)
        self.m0 = w.send(self.own(0), self.at_minus(0), self.minus)

    def mid(self):
        w = self.w
        self.p0.wait_recv()
        self.f0 = w.send(self.near(-1, 0), self.far(-1, 0), self.plus)
        self.m1.wait_recv()
        self.f1 = w.send(self.near(1, 1), self.far(1, 1), self.minus)

    def near_end(self):
        self.p1.wait_recv()
        self.m0.wait_recv()

    def far_end(self):
        self.f0.wait_recv()
        self.f1.wait_recv()


SCRATCH = dict(
    x=((512, 1024), BF),
    c=((512, 1024), BF),
    tk=((256, 1024), BF),
    wu=((1024, 512), BF),
    wd=((512, 1024), BF),
    sstat=((8, 256), F32),
    rstat=((3, 8, 256), F32),
    mean=((256, 128), F32),
    rstd=((256, 128), F32),
    part=((2, 512, 512), BF),
    pa=((2, 4, 256, 128), BF),
    pb=((2, 4, 256, 128), BF),
    pf=((2, 4, 256, 128), BF),
    pg=((2, 4, 256, 128), BF),
    pre=((4, 256, 128), F32),
    hid=((2, 512, 512), BF),
    bs=((2, 256, 1024), BF),
    br=((2, 256, 1024), BF),
    xacc=((2, 256, 1024), F32),
    xown=((2, 4, 16, 1024), F32),
    xs=((2, 4, 4, 16, 1024), BF),
    x1a=((2, 4, 16, 512), BF),
    x1b=((2, 4, 16, 512), BF),
    x2p=((2, 4, 16, 1024), BF),
    x2m=((2, 4, 16, 1024), BF),
    xga=((2, 4, 16, 512), BF),
    xgb=((2, 4, 16, 512), BF),
    zs=((2, 4, 16, 1024), BF),
    z1a=((2, 16, 512), BF),
    z1b=((2, 16, 512), BF),
    z2p=((2, 16, 1024), BF),
    z2m=((2, 16, 1024), BF),
    zga=((2, 16, 512), BF),
    zgb=((2, 16, 512), BF),
    fin=((2, 256, 1024), BF),
    ts=((1, 128), F32),
    tr=((15, 1, 128), F32),
    gdp=((512, 1024), BF),
    gdo=((128, 1024), F32),
    gd1a=((64, 1024), BF),
    gd1b=((64, 1024), BF),
    gd2p=((128, 1024), BF),
    gd2m=((128, 1024), BF),
    gdga=((64, 1024), BF),
    gdgb=((64, 1024), BF),
    gdout=((128, 1024), BF),
    gup=((1024, 512), BF),
    guo=((1024, 128), F32),
    gu1a=((512, 128), BF),
    gu1b=((512, 128), BF),
    gu2p=((1024, 128), BF),
    gu2m=((1024, 128), BF),
    guga=((512, 128), BF),
    gugb=((512, 128), BF),
    guout=((1024, 128), BF),
)
N_SEMS = 224


def rows_of(index, size):
    return pl.ds(pl.multiple_of(index * size, size), size)


def kernel(tok_h, wu_h, wd_h, cot_h, mix_h, ing_h, gu_h, gd_h, *scratch):
    s = dict(zip(SCRATCH, scratch))
    send_sems, recv_sems, local_sems = scratch[len(SCRATCH) :]
    wire = Wire(send_sems, recv_sems)

    fsdp, trow, tcol = lax.axis_index("fsdp"), lax.axis_index("trow"), lax.axis_index("tcol")
    y, core = fsdp // 2, lax.rem(fsdp, 2)
    xx, zh = trow // 4, lax.rem(trow, 4)
    zl = tcol

    def at(dy=0, dcore=0, dx=0, dzh=0):
        return (
            lax.rem(y + dy, 4) * 2 + lax.rem(core + dcore, 2),
            lax.rem(xx + dx, 4) * 4 + lax.rem(zh + dzh, 4),
            tcol,
        )

    def at_zl(index):
        return (fsdp, trow, index)

    partner = at(dcore=1)
    y_plus, y_minus = at(dy=1), at(dy=3)
    x_plus, x_minus = at(dx=1), at(dx=3)
    right = zl // 2
    mate = zl + 1 - 2 * lax.rem(zl, 2)
    far_hub = 2 - right
    is_hub = jnp.logical_or(zl == 1, zl == 2)
    is_end = jnp.logical_or(zl == 0, zl == 3)

    barrier = pltpu.get_barrier_semaphore()
    others = [partner, y_plus, y_minus, x_plus, x_minus]
    for dz in range(4):
        for dl in range(4):
            if dz or dl:
                fs, tr, _ = at(dzh=dz)
                others.append((fs, tr, lax.rem(zl + dl, 4)))
    loads = [
        pltpu.make_async_copy(src, dst, local_sems.at[i])
        for i, (src, dst) in enumerate(
            (
                (tok_h, s["tk"]),
                (wu_h, s["wu"].at[:, 0:128]),
                (wd_h, s["wd"].at[0:128]),
                (cot_h, s["c"].at[0:256]),
            )
        )
    ]
    for load in loads:
        load.start()
    for other in others:
        pl.semaphore_signal(
            barrier, inc=1, device_id=other, device_id_type=pl.DeviceIdType.MESH
        )

    loads[0].wait()
    tok = s["tk"][...].astype(F32)
    sum_one = jnp.sum(tok, axis=1, keepdims=True)
    sum_two = jnp.sum(tok * tok, axis=1, keepdims=True)
    lane = lax.broadcasted_iota(jnp.int32, (256, 128), 1)
    both = jnp.where(lane == 0, sum_one, jnp.where(lane == 1, sum_two, 0.0))
    s["sstat"][...] = jnp.transpose(both)[0:8]
    for load in loads[1:]:
        load.wait()
    pl.semaphore_wait(barrier, len(others))

    def wu_at(pos, h):
        return s["wu"].at[h * 512 : (h + 1) * 512, pos * 128 : (pos + 1) * 128]

    def wd_at(pos, h):
        return s["wd"].at[pos * 128 + h * 64 : pos * 128 + (h + 1) * 64]

    def weights(view):
        return RingCopy(
            wire,
            y_plus,
            y_minus,
            own=lambda h: view(OWN, h),
            at_plus=lambda h: view(PREV, h),
            at_minus=lambda h: view(NEXT, h),
            near=lambda rel, h: view(PREV if rel < 0 else NEXT, h),
            far=lambda rel, h: view(FAR, h),
        )

    ups, downs = weights(wu_at), weights(wd_at)
    ups.start()
    stat_copies = [
        wire.send(s["sstat"], s["rstat"].at[k - 1], at_zl(lax.rem(zl + k, 4))) for k in (1, 2, 3)
    ]
    cot_copy = wire.send(s["c"].at[0:256], s["c"].at[256:512], partner)

    class Exchange:
        def __init__(self, which, pos, first, count):
            self.which, self.first, self.count = which, first, count
            self.lanes = slice(pos * 128, (pos + 1) * 128)
            self.i = (which, pos, slice(first, first + count))
            self.slots = [wire.slot() for _ in range(6)]

        def rows(self, side):
            return pl.ds(pl.multiple_of(side * 256 + self.first, 128), self.count)

        def part(self, side):
            return s["part"].at[self.which, self.rows(side), self.lanes]

        def back(self, side):
            return s["hid"].at[self.which, self.rows(side), self.lanes]

        def start(self):
            far, near = self.slots[0:2]
            to = at_zl(mate)
            self.far = wire.send(self.part(1 - right), s["pb"].at[self.i], to, far, is_end)
            self.near = wire.send(self.part(right), s["pa"].at[self.i], to, near, is_end)

        def mid(self):
            made = wire.copy(s["pg"].at[self.i], s["pf"].at[self.i], at_zl(far_hub), self.slots[2])

            @pl.when(is_hub)
            def _():
                self.far.wait_recv()
                both = self.part(1 - right)[...].astype(F32) + s["pb"][self.i].astype(F32)
                s["pg"][self.i] = both.astype(BF)
                made.start()

            wire.sent.append((made, is_hub))
            self.cross = made

        def end(self, finish):
            mine = self.back(right)
            across = wire.copy(mine, mine, at_zl(far_hub), self.slots[3])
            down = wire.copy(mine, mine, at_zl(mate), self.slots[4])

            @pl.when(is_hub)
            def _():
                self.near.wait_recv()
                self.cross.wait_recv()
                total = self.part(right)[...].astype(F32) + s["pa"][self.i].astype(F32)
                total = total + s["pf"][self.i].astype(F32)
                s["hid"][self.which, self.rows(right), self.lanes] = finish(total, self.i)
                across.start()
                down.start()

            wire.sent += [(across, is_hub), (down, is_hub)]
            self.across, self.down = across, down

        def back_mid(self):
            theirs = self.back(1 - right)
            made = wire.copy(theirs, theirs, at_zl(mate), self.slots[5])

            @pl.when(is_hub)
            def _():
                self.across.wait_recv()
                made.start()

            wire.sent.append((made, is_hub))
            self.passed = made

        def back_end(self):
            @pl.when(is_end)
            def _():
                self.down.wait_recv()
                self.passed.wait_recv()

    def gelu_of(total, i):
        s["pre"][i[1:]] = total
        return gelu_value(total).astype(BF)

    def dpre_of(total, i):
        return (total * gelu_slope(s["pre"][i[1:]])).astype(BF)

    pres = [[Exchange(0, pos, 0, 256)] for pos in range(4)]
    dhs = [[Exchange(1, pos, 0, 256)] for pos in range(3)]
    dhs.append([Exchange(1, 3, 0, 128), Exchange(1, 3, 128, 128)])

    def every(exchanges, step, *args):
        for e in exchanges:
            getattr(e, step)(*args)

    def pre_part(first, last):
        lanes = slice(first * 128, last * 128)
        s["part"][0, :, lanes] = dot(s["x"][...], s["wu"][:, lanes], 1, 0).astype(BF)
        for pos in range(first, last):
            every(pres[pos], "start")

    def dh_part(first, last):
        lanes = slice(first * 128, last * 128)
        s["part"][1, :, lanes] = dot(s["c"][...], s["wd"][lanes], 1, 1).astype(BF)
        for pos in range(first, last):
            every(dhs[pos], "start")

    def pre_done(pos):
        every(pres[pos], "end", gelu_of)

    def dh_done(pos):
        every(dhs[pos], "end", dpre_of)

    cot_copy.wait_recv()
    dh_part(0, 1)

    for c in stat_copies:
        c.wait_recv()
    total = s["sstat"][...] + s["rstat"][0] + s["rstat"][1] + s["rstat"][2]
    total = jnp.transpose(jnp.concatenate([total, jnp.zeros((120, 256), F32)], axis=0))
    mean = total[:, 0:1] / 4096.0
    var = total[:, 1:2] / 4096.0 - mean * mean
    rstd = lax.rsqrt(var + 1e-05)
    s["mean"][...] = jnp.broadcast_to(mean, (256, 128))
    s["rstd"][...] = jnp.broadcast_to(rstd, (256, 128))
    s["x"][0:256] = ((s["tk"][...].astype(F32) - mean) * rstd).astype(BF)
    x_copy = wire.send(s["x"].at[0:256], s["x"].at[256:512], partner)
    ups.mid()
    downs.start()
    x_copy.wait_recv()
    pre_part(0, 1)
    every(dhs[0], "mid")
    ups.near_end()
    pre_part(1, 3)
    every(pres[0], "mid")
    ups.far_end()
    pre_part(3, 4)
    pre_done(0)
    dh_done(0)
    every(pres[1], "mid")
    every(pres[2], "mid")
    downs.mid()
    every(pres[3], "mid")
    every(pres[0], "back_mid")
    every(dhs[0], "back_mid")
    pre_done(1)
    downs.near_end()
    dh_part(1, 3)
    pre_done(2)
    every(pres[1], "back_mid")
    pre_done(3)
    downs.far_end()
    dh_part(3, 4)
    every(dhs[1], "mid")
    every(dhs[2], "mid")
    every(pres[2], "back_mid")
    every(dhs[3], "mid")
    every(pres[3], "back_mid")
    dh_done(1)
    dh_done(2)
    dh_done(3)

    def rows(rel_x, rel_z):
        first = lax.rem(xx + rel_x, 4) * 64 + lax.rem(zh + rel_z, 4) * 16
        return pl.ds(pl.multiple_of(first, 16), 16)

    mine = rows(0, 0)
    steps = (2, 1, 3, 0)
    chunks = (slice(0, 1), slice(1, 4))

    def out_part(o, product):
        s["bs"][o] = product(1).astype(BF)
        sent = []
        for rel in (2, 1, 3, 0):
            r = rows_of(lax.rem(xx + rel, 4), 64)
            sent.append(wire.send(s["bs"].at[o, r], s["br"].at[o, r], partner))
        s["xacc"][o] = product(0)
        return sent

    def over_x(o, k):
        which = pl.ds(chunks[k].start, chunks[k].stop - chunks[k].start)

        def block(rel, h):
            return s["xs"].at[o, which, rel % 4, :, h * 512 : (h + 1) * 512]

        def half(ref, h):
            return ref.at[:, :, h * 512 : (h + 1) * 512]

        names = ("x1a", "x1b", "x2p", "x2m", "xga", "xgb")
        return RingSum(wire, x_plus, x_minus, block, half, [s[n].at[o, which] for n in names])

    x_sums = [[over_x(o, k) for k in (0, 1)] for o in (0, 1)]

    def x_start(o, copies):
        for rel, copy in zip((2, 1, 3, 0), copies):
            copy.wait_recv()
            for k, chunk in enumerate(chunks):
                for i in range(chunk.start, chunk.stop):
                    r = rows(rel, steps[i])
                    value = s["xacc"][o, r] + s["br"][o, r].astype(F32)
                    if rel == 0:
                        s["xown"][o, i] = value
                    else:
                        s["xs"][o, i, rel] = value.astype(BF)
                if rel == 2:
                    x_sums[o][k].start_far()
            if rel == 3:
                x_sums[o][0].start_near()
                x_sums[o][1].start_near()

    def over_z(o):
        def block(rel, h):
            return s["zs"].at[o, rel % 4, :, h * 512 : (h + 1) * 512]

        def half(ref, h):
            return ref.at[:, h * 512 : (h + 1) * 512]

        names = ("z1a", "z1b", "z2p", "z2m", "zga", "zgb")
        return RingSum(wire, at(dzh=1), at(dzh=3), block, half, [s[n].at[o] for n in names])

    z_sums = [over_z(0), over_z(1)]

    def z_start(o, k):
        chunk = chunks[k]
        value = x_sums[o][k].end(s["xown"][o, chunk])
        s["xown"][o, chunk] = value
        for i in range(chunk.start, min(chunk.stop, 3)):
            s["zs"][o, steps[i]] = value[i - chunk.start].astype(BF)
        if k == 0:
            z_sums[o].start_far()
        else:
            z_sums[o].start_near()

    def z_done(o):
        return z_sums[o].end(s["xown"][o, 3])

    def back_z(o):
        def view(rel, h):
            return s["fin"].at[o, rows(0, rel % 4), h * 512 : (h + 1) * 512]

        spread = RingCopy(
            wire,
            at(dzh=1),
            at(dzh=3),
            own=lambda h: view(0, h),
            at_plus=lambda h: view(0, h),
            at_minus=lambda h: view(0, h),
            near=view,
            far=view,
        )
        spread.start()
        return spread

    def back_x(o, rel_z):
        def view(rel, h):
            return s["fin"].at[o, rows(rel % 4, rel_z % 4), h * 512 : (h + 1) * 512]

        return RingCopy(
            wire,
            x_plus,
            x_minus,
            own=lambda h: view(0, h),
            at_plus=lambda h: view(0, h),
            at_minus=lambda h: view(0, h),
            near=view,
            far=view,
        )

    def back_x_start(o, rel_z):
        spread = back_x(o, rel_z)
        spread.start()
        return spread

    pos_of = {1: NEXT, 2: FAR, -1: PREV}

    def gd_block(rel, h):
        first = pos_of[rel] * 128 + h * 64
        return s["gdp"].at[first : first + 64]

    def gu_block(rel, h):
        pos = pos_of[rel]
        return s["gup"].at[h * 512 : (h + 1) * 512, pos * 128 : (pos + 1) * 128]

    gd_names = ("gd1a", "gd1b", "gd2p", "gd2m", "gdga", "gdgb")
    gu_names = ("gu1a", "gu1b", "gu2p", "gu2m", "guga", "gugb")
    gd_sum = RingSum(
        wire, y_plus, y_minus, gd_block, lambda r, h: r.at[h * 64 : (h + 1) * 64],
        [s[n] for n in gd_names],
    )
    gu_sum = RingSum(
        wire, y_plus, y_minus, gu_block, lambda r, h: r.at[h * 512 : (h + 1) * 512],
        [s[n] for n in gu_names],
    )

    for pos in range(4):
        every(pres[pos], "back_end")
    branch_copy = out_part(
        0, lambda half: dot(s["hid"][0, half * 256 : (half + 1) * 256], s["wd"][...], 1, 0)
    )
    every(dhs[1], "back_mid")
    every(dhs[2], "back_mid")
    every(dhs[3], "back_mid")
    x_start(0, branch_copy)
    grad = dot(s["hid"][0], s["c"][...], 0, 0)
    s["gdo"][...] = grad[0:128]
    s["gdp"][128:512] = grad[128:512].astype(BF)
    gd_sum.start()
    for pos in range(4):
        every(dhs[pos], "back_end")

    dnorm_copy = out_part(
        1, lambda half: dot(s["hid"][1, half * 256 : (half + 1) * 256], s["wu"][...], 1, 1)
    )
    x_sums[0][0].mid()
    x_sums[0][1].mid()
    x_start(1, dnorm_copy)
    grad = dot(s["x"][...], s["hid"][1], 0, 0)
    s["guo"][...] = grad[:, 0:128]
    s["gup"][:, 128:512] = grad[:, 128:512].astype(BF)
    gu_sum.start()
    z_start(0, 0)
    z_start(0, 1)
    x_sums[1][0].mid()
    x_sums[1][1].mid()
    gd_sum.mid()
    z_start(1, 0)
    z_start(1, 1)

    lane = lax.broadcasted_iota(jnp.int32, (16, 128), 1)
    row = lax.broadcasted_iota(jnp.int32, (16, 128), 0)
    line = jnp.zeros((1, 128), F32)
    for i in range(4):
        part = s["xown"][1, i]
        r = rows(0, steps[i])
        xhat = (s["tk"][r, :].astype(F32) - s["mean"][r, 0:1]) * s["rstd"][r, 0:1]
        first = jnp.sum(part, axis=1, keepdims=True)
        second = jnp.sum(part * xhat, axis=1, keepdims=True)
        place = row + lax.rem(zh + steps[i], 4) * 16
        spot = jnp.where(lane == place, first, jnp.where(lane == place + 64, second, 0.0))
        line = line + jnp.sum(spot, axis=0, keepdims=True)
    s["ts"][...] = line
    moment_copies = []
    for dz in range(4):
        for dl in range(4):
            if dz or dl:
                fs, tr, _ = at(dzh=dz)
                other = (fs, tr, lax.rem(zl + dl, 4))
                moment_copies.append(wire.send(s["ts"], s["tr"].at[dz * 4 + dl - 1], other))
    z_sums[0].mid()
    gu_sum.mid()
    z_sums[1].mid()
    s["fin"][0, mine, :] = (s["tk"][mine, :].astype(F32) + z_done(0)).astype(BF)
    z_back0 = back_z(0)
    x_backs0 = [back_x_start(0, 0)]
    s["gdout"][...] = gd_sum.end(s["gdo"][...]).astype(BF)
    gd_out = pltpu.make_async_copy(s["gdout"], gd_h, local_sems.at[4])
    gd_out.start()

    dnorm = z_done(1)
    for c in moment_copies:
        c.wait_recv()
    line = s["ts"][...]
    for k in range(15):
        line = line + s["tr"][k]
    place = row + zh * 16
    moment_one = jnp.sum(jnp.where(lane == place, line, 0.0), axis=1, keepdims=True) / 4096.0
    moment_two = jnp.sum(jnp.where(lane == place + 64, line, 0.0), axis=1, keepdims=True) / 4096.0
    rstd = s["rstd"][mine, 0:1]
    xhat = (s["tk"][mine, :].astype(F32) - s["mean"][mine, 0:1]) * rstd
    grad = s["c"][mine, :].astype(F32) + rstd * (dnorm - moment_one - xhat * moment_two)
    s["fin"][1, mine, :] = grad.astype(BF)
    z_back1 = back_z(1)
    x_backs1 = [back_x_start(1, 0)]
    z_back0.mid()
    z_back0.near_end()
    x_backs0 += [back_x_start(0, 1), back_x_start(0, 3)]
    x_backs0[0].mid()
    x_backs1[0].mid()
    z_back1.mid()
    z_back1.near_end()
    x_backs1 += [back_x_start(1, 1), back_x_start(1, 3)]
    x_backs0[1].mid()
    x_backs0[2].mid()
    z_back0.far_end()
    x_backs0.append(back_x_start(0, 2))
    x_backs1[1].mid()
    x_backs1[2].mid()
    s["guout"][...] = gu_sum.end(s["guo"][...]).astype(BF)
    gu_out = pltpu.make_async_copy(s["guout"], gu_h, local_sems.at[5])
    gu_out.start()
    x_backs0[3].mid()
    z_back1.far_end()
    x_backs1.append(back_x_start(1, 2))
    for spread in x_backs0:
        spread.near_end()
        spread.far_end()
    mix_out = pltpu.make_async_copy(s["fin"].at[0], mix_h, local_sems.at[6])
    mix_out.start()
    x_backs1[3].mid()
    for spread in x_backs1:
        spread.near_end()
        spread.far_end()
    ing_out = pltpu.make_async_copy(s["fin"].at[1], ing_h, local_sems.at[7])
    ing_out.start()
    wire.drain()
    assert wire.count <= N_SEMS, wire.count
    for out in (gd_out, gu_out, mix_out, ing_out):
        out.wait()


def hand_over(*refs):
    sems = refs[-1]
    copies = [pltpu.make_async_copy(refs[i], refs[4 + i], sems.at[i]) for i in range(4)]
    for c in copies:
        c.start()
    for c in copies:
        c.wait()


def local(tokens, w_up, w_down, cotangent):
    scratch = [pltpu.VMEM(shape, dtype) for shape, dtype in SCRATCH.values()]
    scratch += [pltpu.SemaphoreType.DMA((N_SEMS,)), pltpu.SemaphoreType.DMA((N_SEMS,))]
    scratch += [pltpu.SemaphoreType.DMA((8,))]
    outs = (
        jax.ShapeDtypeStruct(tokens.shape, BF),
        jax.ShapeDtypeStruct(cotangent.shape, BF),
        jax.ShapeDtypeStruct(w_up.shape, BF),
        jax.ShapeDtypeStruct(w_down.shape, BF),
    )
    tokens, w_up, w_down, cotangent = (
        pltpu.with_memory_space_constraint(a, pltpu.HBM)
        for a in (tokens, w_up, w_down, cotangent)
    )
    made = pl.pallas_call(
        kernel,
        out_shape=outs,
        in_specs=[pl.BlockSpec(memory_space=pltpu.HBM)] * 4,
        out_specs=[pl.BlockSpec(memory_space=pl.ANY)] * 4,
        scratch_shapes=scratch,
        compiler_params=pltpu.CompilerParams(
            collective_id=0, has_side_effects=True, vmem_limit_bytes=32 * 1024 * 1024
        ),
        name="block",
    )(tokens, w_up, w_down, cotangent)
    return pl.pallas_call(
        hand_over,
        out_shape=outs,
        in_specs=[pl.BlockSpec(memory_space=pl.ANY)] * 4,
        out_specs=[pl.BlockSpec(memory_space=pl.ANY)] * 4,
        scratch_shapes=[pltpu.SemaphoreType.DMA((4,))],
        compiler_params=pltpu.CompilerParams(vmem_limit_bytes=1024 * 1024),
        name="hand_over",
    )(*made)


def solution(mesh):
    return jax.shard_map(
        local,
        mesh=mesh,
        in_specs=(
            P("fsdp", "tcol"),
            P("tcol", ("fsdp", "trow")),
            P(("fsdp", "trow"), "tcol"),
            P("fsdp", "tcol"),
        ),
        out_specs=(
            P("fsdp", "tcol"),
            P("fsdp", "tcol"),
            P("tcol", ("fsdp", "trow")),
            P(("fsdp", "trow"), "tcol"),
        ),
        check_vma=False,
    )
```

```python
import jax
import jax.numpy as jnp
from jax import lax
from jax.experimental import pallas as pl
from jax.experimental.pallas import tpu as pltpu
from jax.sharding import PartitionSpec as P

BF = jnp.bfloat16
F32 = jnp.float32
OWN, PREV, NEXT, FAR = 0, 1, 2, 3


def gelu_value(pre):
    phi = 0.5 * (1.0 + lax.erf(pre * 0.7071067811865476))
    return pre * phi


def gelu_slope(pre):
    phi = 0.5 * (1.0 + lax.erf(pre * 0.7071067811865476))
    return phi + pre * jnp.exp(-0.5 * pre * pre) * 0.3989422804014327


def dot(left, right, left_dim, right_dim):
    return lax.dot_general(
        left, right, (((left_dim,), (right_dim,)), ((), ())), preferred_element_type=F32
    )


class Wire:
    def __init__(self, send_sems, recv_sems):
        self.send_sems, self.recv_sems = send_sems, recv_sems
        self.count = 0
        self.turn = 0
        self.last = {}

    def slot(self):
        self.count += 1
        return self.count - 1

    def copy(self, src, dst, device, slot):
        turn = self.turn % N_SENDS
        self.turn += 1
        made = pltpu.make_async_remote_copy(
            src_ref=src,
            dst_ref=dst,
            send_sem=self.send_sems.at[turn],
            recv_sem=self.recv_sems.at[slot],
            device_id=device,
            device_id_type=pl.DeviceIdType.MESH,
        )
        self.finish(turn)
        return made, turn

    def finish(self, turn):
        if turn in self.last:
            made, when = self.last.pop(turn)
            if when is None:
                made.wait_send()
            else:
                pl.when(when)(made.wait_send)

    def started(self, pair, when=None):
        self.last[pair[1]] = (pair[0], when)

    def send(self, src, dst, device, slot=None, when=None):
        pair = self.copy(src, dst, device, self.slot() if slot is None else slot)
        if when is None:
            pair[0].start()
        else:
            pl.when(when)(pair[0].start)
        self.started(pair, when)
        return pair[0]

    def wait_for(self, ref, slot):
        pltpu.make_async_copy(ref, ref, self.recv_sems.at[slot]).wait()

    def drain(self):
        for turn in list(self.last):
            self.finish(turn)


class RingSum:
    def __init__(self, wire, plus, minus, block, half, bufs):
        self.w, self.plus, self.minus, self.block, self.half = wire, plus, minus, block, half
        self.r1a, self.r1b, self.r2p, self.r2m, self.ga, self.gb = bufs

    def start(self):
        self.start_far()
        self.start_near()

    def start_far(self):
        w = self.w
        self.c1 = w.send(self.block(2, 0), self.r1a, self.plus)
        self.c2 = w.send(self.block(2, 1), self.r1b, self.minus)

    def start_near(self):
        w, half = self.w, self.half
        self.sp, self.sm = w.slot(), w.slot()
        w.send(self.block(1, 1), half(self.r2p, 1), self.plus, self.sp)
        w.send(self.block(-1, 0), half(self.r2m, 0), self.minus, self.sm)

    def mid(self):
        w, half = self.w, self.half
        self.c1.wait_recv()
        self.ga[...] = (self.block(1, 0)[...].astype(F32) + self.r1a[...].astype(F32)).astype(BF)
        w.send(self.ga, half(self.r2p, 0), self.plus, self.sp)
        self.c2.wait_recv()
        self.gb[...] = (self.block(-1, 1)[...].astype(F32) + self.r1b[...].astype(F32)).astype(BF)
        w.send(self.gb, half(self.r2m, 1), self.minus, self.sm)

    def end(self, own):
        self.w.wait_for(self.r2p, self.sp)
        self.w.wait_for(self.r2m, self.sm)
        return own + self.r2p[...].astype(F32) + self.r2m[...].astype(F32)


class RingCopy:
    def __init__(self, wire, plus, minus, own, at_plus, at_minus, near, far):
        self.w, self.plus, self.minus = wire, plus, minus
        self.own, self.at_plus, self.at_minus, self.near, self.far = own, at_plus, at_minus, near, far

    def start(self):
        w = self.w
        self.p0 = w.send(self.own(0), self.at_plus(0), self.plus)
        self.m1 = w.send(self.own(1), self.at_minus(1), self.minus)
        self.p1 = w.send(self.own(1), self.at_plus(1), self.plus)
        self.m0 = w.send(self.own(0), self.at_minus(0), self.minus)

    def mid(self):
        w = self.w
        self.p0.wait_recv()
        self.f0 = w.send(self.near(-1, 0), self.far(-1, 0), self.plus)
        self.m1.wait_recv()
        self.f1 = w.send(self.near(1, 1), self.far(1, 1), self.minus)

    def near_end(self):
        self.p1.wait_recv()
        self.m0.wait_recv()

    def far_end(self):
        self.f0.wait_recv()
        self.f1.wait_recv()


class BlockCopy:
    def __init__(self, wire, plus, minus, view, whole):
        self.w, self.plus, self.minus, self.view, self.whole = wire, plus, minus, view, whole

    def start(self):
        w, mine = self.w, self.whole(0)
        self.p = w.send(mine, mine, self.plus)
        self.m = w.send(mine, mine, self.minus)
        self.slot = w.slot()

    def mid(self):
        w = self.w
        self.p.wait_recv()
        half = self.view(-1, 0)
        w.send(half, half, self.plus, self.slot)
        self.m.wait_recv()
        half = self.view(1, 1)
        w.send(half, half, self.minus, self.slot)

    def end(self):
        self.w.wait_for(self.whole(2), self.slot)


SCRATCH = dict(
    x=((512, 1024), BF),
    c=((512, 1024), BF),
    tk=((256, 1024), BF),
    wu=((4, 1024, 128), BF),
    wd=((512, 1024), BF),
    sstat=((8, 256), F32),
    rstat=((3, 8, 256), F32),
    mean=((256, 128), F32),
    rstd=((256, 128), F32),
    part=((2, 4, 512, 128), BF),
    pa=((2, 4, 256, 128), BF),
    pb=((2, 4, 256, 128), BF),
    pf=((2, 4, 256, 128), BF),
    pg=((2, 4, 256, 128), BF),
    pre=((4, 256, 128), F32),
    hid=((2, 4, 512, 128), BF),
    bs=((2, 256, 1024), BF),
    br=((2, 256, 1024), BF),
    xacc=((2, 256, 1024), F32),
    xown=((2, 4, 16, 1024), F32),
    xs=((2, 4, 4, 16, 1024), BF),
    x1a=((2, 4, 16, 512), BF),
    x1b=((2, 4, 16, 512), BF),
    x2p=((2, 4, 16, 1024), BF),
    x2m=((2, 4, 16, 1024), BF),
    xga=((2, 4, 16, 512), BF),
    xgb=((2, 4, 16, 512), BF),
    zs=((2, 4, 16, 1024), BF),
    z1a=((2, 16, 512), BF),
    z1b=((2, 16, 512), BF),
    z2p=((2, 16, 1024), BF),
    z2m=((2, 16, 1024), BF),
    zga=((2, 16, 512), BF),
    zgb=((2, 16, 512), BF),
    fin=((2, 256, 1024), BF),
    ts=((1, 128), F32),
    tr=((3, 1, 128), F32),
    tz=((4, 1, 128), F32),
    gdp=((512, 1024), BF),
    gdo=((128, 1024), F32),
    gd1a=((64, 1024), BF),
    gd1b=((64, 1024), BF),
    gd2p=((128, 1024), BF),
    gd2m=((128, 1024), BF),
    gdga=((64, 1024), BF),
    gdgb=((64, 1024), BF),
    gdout=((128, 1024), BF),
    gup=((4, 1024, 128), BF),
    guo=((1024, 128), F32),
    gu1a=((512, 128), BF),
    gu1b=((512, 128), BF),
    gu2p=((1024, 128), BF),
    gu2m=((1024, 128), BF),
    guga=((512, 128), BF),
    gugb=((512, 128), BF),
    guout=((1024, 128), BF),
)
N_SEMS = 149
N_SENDS = 32


def rows_of(index, size):
    return pl.ds(pl.multiple_of(index * size, size), size)


def kernel(tok_h, wu_h, wd_h, cot_h, mix_h, ing_h, gu_h, gd_h, *scratch):
    s = dict(zip(SCRATCH, scratch))
    send_sems, recv_sems, local_sems = scratch[len(SCRATCH) :]
    wire = Wire(send_sems, recv_sems)

    fsdp, trow, tcol = lax.axis_index("fsdp"), lax.axis_index("trow"), lax.axis_index("tcol")
    y, core = fsdp // 2, lax.rem(fsdp, 2)
    xx, zh = trow // 4, lax.rem(trow, 4)
    zl = tcol

    def at(dy=0, dcore=0, dx=0, dzh=0):
        return (
            lax.rem(y + dy, 4) * 2 + lax.rem(core + dcore, 2),
            lax.rem(xx + dx, 4) * 4 + lax.rem(zh + dzh, 4),
            tcol,
        )

    def at_zl(index):
        return (fsdp, trow, index)

    partner = at(dcore=1)
    y_plus, y_minus = at(dy=1), at(dy=3)
    x_plus, x_minus = at(dx=1), at(dx=3)
    right = zl // 2
    mate = zl + 1 - 2 * lax.rem(zl, 2)
    far_hub = 2 - right
    far_end = 3 - 3 * right
    is_hub = jnp.logical_or(zl == 1, zl == 2)
    is_end = jnp.logical_or(zl == 0, zl == 3)

    barrier = pltpu.get_barrier_semaphore()
    z_plus, z_minus = at(dzh=1), at(dzh=3)
    others = [partner, y_plus, y_minus, x_plus, x_minus, z_plus, z_minus]
    others += [at_zl(lax.rem(zl + k, 4)) for k in (1, 2, 3)]
    loads = [
        pltpu.make_async_copy(src, dst, local_sems.at[i])
        for i, (src, dst) in enumerate(
            (
                (tok_h, s["tk"]),
                (wu_h, s["wu"].at[0]),
                (wd_h, s["wd"].at[0:128]),
                (cot_h, s["c"].at[0:256]),
            )
        )
    ]
    for load in loads:
        load.start()
    for other in others:
        pl.semaphore_signal(
            barrier, inc=1, device_id=other, device_id_type=pl.DeviceIdType.MESH
        )

    loads[0].wait()
    tok = s["tk"][...].astype(F32)
    sum_one = jnp.sum(tok, axis=1, keepdims=True)
    sum_two = jnp.sum(tok * tok, axis=1, keepdims=True)
    lane = lax.broadcasted_iota(jnp.int32, (256, 128), 1)
    both = jnp.where(lane == 0, sum_one, jnp.where(lane == 1, sum_two, 0.0))
    s["sstat"][...] = jnp.transpose(both)[0:8]
    for load in loads[1:]:
        load.wait()
    pl.semaphore_wait(barrier, len(others))

    def wu_at(pos, h):
        return s["wu"].at[pos, h * 512 : (h + 1) * 512]

    def wd_at(pos, h):
        return s["wd"].at[pos * 128 + h * 64 : pos * 128 + (h + 1) * 64]

    def weights(view):
        return RingCopy(
            wire,
            y_plus,
            y_minus,
            own=lambda h: view(OWN, h),
            at_plus=lambda h: view(PREV, h),
            at_minus=lambda h: view(NEXT, h),
            near=lambda rel, h: view(PREV if rel < 0 else NEXT, h),
            far=lambda rel, h: view(FAR, h),
        )

    ups, downs = weights(wu_at), weights(wd_at)
    ups.start()
    stat_slot = wire.slot()
    for k in (1, 2, 3):
        wire.send(s["sstat"], s["rstat"].at[k - 1], at_zl(lax.rem(zl + k, 4)), stat_slot)
    cot_copy = wire.send(s["c"].at[0:256], s["c"].at[256:512], partner)

    class Exchange:
        def __init__(self, which, pos, first, count):
            self.which, self.first, self.count = which, first, count
            self.pos = pos
            self.i = (which, pos, slice(first, first + count))
            self.slots = [wire.slot() for _ in range(6)]

        def rows(self, side):
            if isinstance(side, int):
                return pl.ds(side * 256 + self.first, self.count)
            return pl.ds(pl.multiple_of(side * 256 + self.first, 128), self.count)

        def part(self, side):
            return s["part"].at[self.which, self.pos, self.rows(side)]

        def back(self, side):
            return s["hid"].at[self.which, self.pos, self.rows(side)]

        def start(self):
            self.far = wire.send(
                self.part(1 - right), s["pb"].at[self.i], at_zl(mate), self.slots[0], is_end
            )

        def start_side(self, side):
            to, part, (far, near) = at_zl(mate), self.part(side), self.slots[0:2]
            self.near = wire.send(part, s["pa"].at[self.i], to, near, zl == 3 * side)
            self.far = wire.send(part, s["pb"].at[self.i], to, far, zl == 3 - 3 * side)

        def start_near(self):
            self.near = wire.send(
                self.part(right), s["pa"].at[self.i], at_zl(mate), self.slots[1], is_end
            )

        def mid(self):
            pair = wire.copy(s["pg"].at[self.i], s["pf"].at[self.i], at_zl(far_hub), self.slots[2])

            @pl.when(is_hub)
            def _():
                self.far.wait_recv()
                both = self.part(1 - right)[...].astype(F32) + s["pb"][self.i].astype(F32)
                s["pg"][self.i] = both.astype(BF)
                pair[0].start()

            wire.started(pair, is_hub)
            self.cross = pair[0]

        def end(self, finish):
            mine = self.back(right)
            across = wire.copy(mine, mine, at_zl(far_hub), self.slots[3])
            down = wire.copy(mine, mine, at_zl(mate), self.slots[4])

            @pl.when(is_hub)
            def _():
                self.near.wait_recv()
                self.cross.wait_recv()
                total = self.part(right)[...].astype(F32) + s["pa"][self.i].astype(F32)
                total = total + s["pf"][self.i].astype(F32)
                s["hid"][self.which, self.pos, self.rows(right)] = finish(total, self.i)
                across[0].start()
                down[0].start()

            wire.started(across, is_hub)
            wire.started(down, is_hub)
            self.across, self.down = across[0], down[0]

        def back_mid(self):
            theirs = self.back(1 - right)
            pair = wire.copy(theirs, theirs, at_zl(mate), self.slots[5])

            @pl.when(is_hub)
            def _():
                self.across.wait_recv()
                pair[0].start()

            wire.started(pair, is_hub)
            self.passed = pair[0]

        def back_end(self):
            @pl.when(is_end)
            def _():
                self.down.wait_recv()
                self.passed.wait_recv()

    class LastExchange(Exchange):
        def end(self, finish):
            mine = self.back(right)
            beyond = wire.copy(mine, mine, at_zl(far_end), self.slots[5])
            across = wire.copy(mine, mine, at_zl(far_hub), self.slots[3])
            down = wire.copy(mine, mine, at_zl(mate), self.slots[4])

            @pl.when(is_hub)
            def _():
                self.near.wait_recv()
                self.cross.wait_recv()
                total = self.part(right)[...].astype(F32) + s["pa"][self.i].astype(F32)
                total = total + s["pf"][self.i].astype(F32)
                s["hid"][self.which, self.pos, self.rows(right)] = finish(total, self.i)
                beyond[0].start()
                across[0].start()
                down[0].start()

            for pair in (beyond, across, down):
                wire.started(pair, is_hub)
            self.passed, self.across, self.down = beyond[0], across[0], down[0]

        def back_mid(self):
            pl.when(is_hub)(self.across.wait_recv)

    def gelu_of(total, i):
        s["pre"][i[1:]] = total
        return gelu_value(total).astype(BF)

    def dpre_of(total, i):
        return (total * gelu_slope(s["pre"][i[1:]])).astype(BF)

    pres = [[Exchange(0, pos, 0, 256)] for pos in range(4)]
    dhs = [[Exchange(1, pos, 0, 256)] for pos in range(3)]
    dhs.append([LastExchange(1, 3, 0, 128), LastExchange(1, 3, 128, 128)])

    def every(exchanges, step, *args):
        for e in exchanges:
            getattr(e, step)(*args)

    def side_by_side(blocks):
        return blocks[0] if len(blocks) == 1 else jnp.concatenate(blocks, axis=1)

    def put_part(which, first, last, value):
        for pos in range(first, last):
            lanes = slice((pos - first) * 128, (pos - first + 1) * 128)
            s["part"][which, pos] = value[:, lanes].astype(BF)

    def pre_part(first, last):
        blocks = side_by_side([s["wu"][pos] for pos in range(first, last)])
        put_part(0, first, last, dot(s["x"][...], blocks, 1, 0))
        for step in ("start", "start_near"):
            for pos in range(first, last):
                every(pres[pos], step)

    def dh_part(first, last):
        lanes = slice(first * 128, last * 128)
        put_part(1, first, last, dot(s["c"][...], s["wd"][lanes], 1, 1))
        for step in ("start", "start_near"):
            for pos in range(first, last):
                every(dhs[pos], step)

    def pre_done(pos):
        every(pres[pos], "end", gelu_of)

    def dh_done(pos):
        every(dhs[pos], "end", dpre_of)

    def own_block(which, side, value):
        s["part"][which, 0, side * 256 : (side + 1) * 256] = value.astype(BF)
        every((pres, dhs)[which][0], "start_side", side)

    own_block(1, 0, dot(s["c"][0:256], s["wd"][0:128], 1, 1))
    cot_copy.wait_recv()
    own_block(1, 1, dot(s["c"][256:512], s["wd"][0:128], 1, 1))

    wire.wait_for(s["rstat"], stat_slot)
    total = s["sstat"][...] + s["rstat"][0] + s["rstat"][1] + s["rstat"][2]
    total = jnp.transpose(jnp.concatenate([total, jnp.zeros((120, 256), F32)], axis=0))
    mean = total[:, 0:1] / 4096.0
    var = total[:, 1:2] / 4096.0 - mean * mean
    rstd = lax.rsqrt(var + 1e-05)
    s["mean"][...] = jnp.broadcast_to(mean, (256, 128))
    s["rstd"][...] = jnp.broadcast_to(rstd, (256, 128))
    s["x"][0:256] = ((s["tk"][...].astype(F32) - mean) * rstd).astype(BF)
    x_copy = wire.send(s["x"].at[0:256], s["x"].at[256:512], partner)
    own_block(0, 0, dot(s["x"][0:256], s["wu"][0], 1, 0))
    ups.mid()
    downs.start()
    x_copy.wait_recv()
    own_block(0, 1, dot(s["x"][256:512], s["wu"][0], 1, 0))
    every(dhs[0], "mid")
    ups.near_end()
    pre_part(1, 3)
    every(pres[0], "mid")
    ups.far_end()
    pre_part(3, 4)
    pre_done(0)
    dh_done(0)
    every(pres[1], "mid")
    every(pres[2], "mid")
    downs.mid()
    every(pres[3], "mid")
    every(pres[0], "back_mid")
    every(dhs[0], "back_mid")
    downs.near_end()
    dh_part(1, 3)
    pre_done(1)
    pre_done(2)
    every(dhs[1], "mid")
    downs.far_end()
    dh_part(3, 4)
    every(dhs[2], "mid")
    pre_done(3)
    every(pres[1], "back_mid")
    every(pres[2], "back_mid")
    dh_done(1)
    every(pres[3], "back_mid")
    every(dhs[3], "mid")
    dh_done(2)
    every(dhs[1], "back_mid")

    def rows(rel_x, rel_z):
        first = lax.rem(xx + rel_x, 4) * 64 + lax.rem(zh + rel_z, 4) * 16
        return pl.ds(pl.multiple_of(first, 16), 16)

    mine = rows(0, 0)
    steps = (2, 1, 3, 0)
    chunks = (slice(0, 1), slice(1, 4))

    def out_part(o, product):
        s["bs"][o] = product(1).astype(BF)
        sent = []
        for rel in (2, 1, 3, 0):
            r = rows_of(lax.rem(xx + rel, 4), 64)
            sent.append(wire.send(s["bs"].at[o, r], s["br"].at[o, r], partner))
        s["xacc"][o] = product(0)
        return sent

    def over_x(o, k):
        which = pl.ds(chunks[k].start, chunks[k].stop - chunks[k].start)

        def block(rel, h):
            return s["xs"].at[o, which, rel % 4, :, h * 512 : (h + 1) * 512]

        def half(ref, h):
            return ref.at[:, :, h * 512 : (h + 1) * 512]

        names = ("x1a", "x1b", "x2p", "x2m", "xga", "xgb")
        return RingSum(wire, x_plus, x_minus, block, half, [s[n].at[o, which] for n in names])

    x_sums = [[over_x(o, k) for k in (0, 1)] for o in (0, 1)]

    def x_start(o, copies):
        for rel, copy in zip((2, 1, 3, 0), copies):
            copy.wait_recv()
            for k, chunk in enumerate(chunks):
                for i in range(chunk.start, chunk.stop):
                    r = rows(rel, steps[i])
                    value = s["xacc"][o, r] + s["br"][o, r].astype(F32)
                    if rel == 0:
                        s["xown"][o, i] = value
                    else:
                        s["xs"][o, i, rel] = value.astype(BF)
                if rel == 2:
                    x_sums[o][k].start_far()
            if rel == 3:
                x_sums[o][0].start_near()
                x_sums[o][1].start_near()

    def over_z(o):
        def block(rel, h):
            return s["zs"].at[o, rel % 4, :, h * 512 : (h + 1) * 512]

        def half(ref, h):
            return ref.at[:, h * 512 : (h + 1) * 512]

        names = ("z1a", "z1b", "z2p", "z2m", "zga", "zgb")
        return RingSum(wire, at(dzh=1), at(dzh=3), block, half, [s[n].at[o] for n in names])

    z_sums = [over_z(0), over_z(1)]

    def z_start(o, k):
        chunk = chunks[k]
        value = x_sums[o][k].end(s["xown"][o, chunk])
        s["xown"][o, chunk] = value
        for i in range(chunk.start, min(chunk.stop, 3)):
            s["zs"][o, steps[i]] = value[i - chunk.start].astype(BF)
        if k == 0:
            z_sums[o].start_far()
        else:
            z_sums[o].start_near()

    def z_done(o):
        return z_sums[o].end(s["xown"][o, 3])

    def back_z(o):
        def view(rel, h):
            return s["fin"].at[o, rows(0, rel % 4), h * 512 : (h + 1) * 512]

        spread = RingCopy(
            wire,
            at(dzh=1),
            at(dzh=3),
            own=lambda h: view(0, h),
            at_plus=lambda h: view(0, h),
            at_minus=lambda h: view(0, h),
            near=view,
            far=view,
        )
        spread.start()
        return spread

    def back_x(o, rel_z):
        def view(rel, h):
            return s["fin"].at[o, rows(rel % 4, rel_z % 4), h * 512 : (h + 1) * 512]

        def whole(rel):
            return s["fin"].at[o, rows(rel % 4, rel_z % 4)]

        return BlockCopy(wire, x_plus, x_minus, view, whole)

    def back_x_start(o, rel_z):
        spread = back_x(o, rel_z)
        spread.start()
        return spread

    pos_of = {1: NEXT, 2: FAR, -1: PREV}

    def gd_block(rel, h):
        first = pos_of[rel] * 128 + h * 64
        return s["gdp"].at[first : first + 64]

    def gu_block(rel, h):
        pos = pos_of[rel]
        return s["gup"].at[pos, h * 512 : (h + 1) * 512]

    gd_names = ("gd1a", "gd1b", "gd2p", "gd2m", "gdga", "gdgb")
    gu_names = ("gu1a", "gu1b", "gu2p", "gu2m", "guga", "gugb")
    gd_sum = RingSum(
        wire, y_plus, y_minus, gd_block, lambda r, h: r.at[h * 64 : (h + 1) * 64],
        [s[n] for n in gd_names],
    )
    gu_sum = RingSum(
        wire, y_plus, y_minus, gu_block, lambda r, h: r.at[h * 512 : (h + 1) * 512],
        [s[n] for n in gu_names],
    )

    def hid(which, first, last):
        return side_by_side([s["hid"][which, pos, first:last] for pos in range(4)])

    for pos in range(4):
        every(pres[pos], "back_end")
    branch_copy = out_part(
        0, lambda half: dot(hid(0, half * 256, half * 256 + 256), s["wd"][...], 1, 0)
    )
    dh_done(3)
    every(dhs[2], "back_mid")
    x_start(0, branch_copy)
    grad = dot(hid(0, 0, 512), s["c"][...], 0, 0)
    s["gdo"][...] = grad[0:128]
    s["gdp"][128:512] = grad[128:512].astype(BF)
    gd_sum.start()
    every(dhs[3], "back_mid")
    x_sums[0][0].mid()
    x_sums[0][1].mid()
    for pos in range(4):
        every(dhs[pos], "back_end")

    dnorm_copy = out_part(
        1,
        lambda half: dot(
            hid(1, half * 256, half * 256 + 256),
            side_by_side([s["wu"][pos] for pos in range(4)]),
            1,
            1,
        ),
    )
    z_start(0, 0)
    x_start(1, dnorm_copy)
    z_start(0, 1)
    grad = dot(s["x"][...], hid(1, 0, 512), 0, 0)
    s["guo"][...] = grad[:, 0:128]
    for pos in (1, 2, 3):
        s["gup"][pos] = grad[:, pos * 128 : (pos + 1) * 128].astype(BF)
    gu_sum.start()
    x_sums[1][0].mid()
    x_sums[1][1].mid()
    gd_sum.mid()
    z_start(1, 0)
    z_start(1, 1)

    z_sums[0].mid()

    lane = lax.broadcasted_iota(jnp.int32, (16, 128), 1)
    row = lax.broadcasted_iota(jnp.int32, (16, 128), 0)
    line = jnp.zeros((1, 128), F32)
    for i in range(4):
        part = s["xown"][1, i]
        r = rows(0, steps[i])
        xhat = (s["tk"][r, :].astype(F32) - s["mean"][r, 0:1]) * s["rstd"][r, 0:1]
        first = jnp.sum(part, axis=1, keepdims=True)
        second = jnp.sum(part * xhat, axis=1, keepdims=True)
        place = row + lax.rem(zh + steps[i], 4) * 16
        spot = jnp.where(lane == place, first, jnp.where(lane == place + 64, second, 0.0))
        line = line + jnp.sum(spot, axis=0, keepdims=True)
    s["ts"][...] = line
    moment_slot = wire.slot()
    for k in (1, 2, 3):
        wire.send(s["ts"], s["tr"].at[k - 1], at_zl(lax.rem(zl + k, 4)), moment_slot)
    gu_sum.mid()
    wire.wait_for(s["tr"], moment_slot)
    s["tz"][0] = s["ts"][...] + s["tr"][0] + s["tr"][1] + s["tr"][2]
    moment_copies = [
        wire.send(s["tz"].at[0], s["tz"].at[d], at(dzh=d)) for d in (2, 1, 3)
    ]
    z_sums[1].mid()
    s["fin"][0, mine, :] = (s["tk"][mine, :].astype(F32) + z_done(0)).astype(BF)
    z_back0 = back_z(0)
    x_backs0 = [back_x_start(0, 0)]
    s["gdout"][...] = gd_sum.end(s["gdo"][...]).astype(BF)
    gd_out = pltpu.make_async_copy(s["gdout"], gd_h, local_sems.at[4])
    gd_out.start()

    dnorm = z_done(1)
    for c in moment_copies:
        c.wait_recv()
    line = s["tz"][0] + s["tz"][1] + s["tz"][2] + s["tz"][3]
    place = row + zh * 16
    moment_one = jnp.sum(jnp.where(lane == place, line, 0.0), axis=1, keepdims=True) / 4096.0
    moment_two = jnp.sum(jnp.where(lane == place + 64, line, 0.0), axis=1, keepdims=True) / 4096.0
    rstd = s["rstd"][mine, 0:1]
    xhat = (s["tk"][mine, :].astype(F32) - s["mean"][mine, 0:1]) * rstd
    grad = s["c"][mine, :].astype(F32) + rstd * (dnorm - moment_one - xhat * moment_two)
    s["fin"][1, mine, :] = grad.astype(BF)
    z_back1 = back_z(1)
    x_backs1 = [back_x_start(1, 0)]
    x_backs0[0].mid()
    z_back0.mid()
    z_back0.near_end()
    x_backs0 += [back_x_start(0, 1), back_x_start(0, 3)]
    x_backs1[0].mid()
    x_backs0[1].mid()
    x_backs0[2].mid()
    z_back0.far_end()
    x_backs0.append(back_x_start(0, 2))
    z_back1.mid()
    z_back1.near_end()
    x_backs1 += [back_x_start(1, 1), back_x_start(1, 3)]
    s["guout"][...] = gu_sum.end(s["guo"][...]).astype(BF)
    gu_out = pltpu.make_async_copy(s["guout"], gu_h, local_sems.at[5])
    gu_out.start()
    x_backs1[1].mid()
    x_backs1[2].mid()
    x_backs0[3].mid()
    z_back1.far_end()
    x_backs1.append(back_x_start(1, 2))
    for spread in x_backs0:
        spread.end()
    mix_out = pltpu.make_async_copy(s["fin"].at[0], mix_h, local_sems.at[6])
    mix_out.start()
    x_backs1[3].mid()
    for spread in x_backs1:
        spread.end()
    ing_out = pltpu.make_async_copy(s["fin"].at[1], ing_h, local_sems.at[7])
    ing_out.start()
    wire.drain()
    assert wire.count == N_SEMS, wire.count
    for out in (gd_out, gu_out, mix_out, ing_out):
        out.wait()


def hand_over(*refs):
    sems = refs[-1]
    copies = [pltpu.make_async_copy(refs[i], refs[4 + i], sems.at[i]) for i in range(4)]
    for c in copies:
        c.start()
    for c in copies:
        c.wait()


def local(tokens, w_up, w_down, cotangent):
    scratch = [pltpu.VMEM(shape, dtype) for shape, dtype in SCRATCH.values()]
    scratch += [pltpu.SemaphoreType.DMA((N_SENDS,)), pltpu.SemaphoreType.DMA((N_SEMS,))]
    scratch += [pltpu.SemaphoreType.DMA((8,))]
    outs = (
        jax.ShapeDtypeStruct(tokens.shape, BF),
        jax.ShapeDtypeStruct(cotangent.shape, BF),
        jax.ShapeDtypeStruct(w_up.shape, BF),
        jax.ShapeDtypeStruct(w_down.shape, BF),
    )
    tokens, w_up, w_down, cotangent = (
        pltpu.with_memory_space_constraint(a, pltpu.HBM)
        for a in (tokens, w_up, w_down, cotangent)
    )
    made = pl.pallas_call(
        kernel,
        out_shape=outs,
        in_specs=[pl.BlockSpec(memory_space=pltpu.HBM)] * 4,
        out_specs=[pl.BlockSpec(memory_space=pl.ANY)] * 4,
        scratch_shapes=scratch,
        compiler_params=pltpu.CompilerParams(
            collective_id=0, has_side_effects=True, vmem_limit_bytes=32 * 1024 * 1024
        ),
        name="block",
    )(tokens, w_up, w_down, cotangent)
    return pl.pallas_call(
        hand_over,
        out_shape=outs,
        in_specs=[pl.BlockSpec(memory_space=pl.ANY)] * 4,
        out_specs=[pl.BlockSpec(memory_space=pl.ANY)] * 4,
        scratch_shapes=[pltpu.SemaphoreType.DMA((4,))],
        compiler_params=pltpu.CompilerParams(vmem_limit_bytes=1024 * 1024),
        name="hand_over",
    )(*made)


def solution(mesh):
    return jax.shard_map(
        local,
        mesh=mesh,
        in_specs=(
            P("fsdp", "tcol"),
            P("tcol", ("fsdp", "trow")),
            P(("fsdp", "trow"), "tcol"),
            P("fsdp", "tcol"),
        ),
        out_specs=(
            P("fsdp", "tcol"),
            P("fsdp", "tcol"),
            P("tcol", ("fsdp", "trow")),
            P(("fsdp", "trow"), "tcol"),
        ),
        check_vma=False,
    )
```

```python
import jax
import jax.numpy as jnp
from jax import lax
from jax.experimental import pallas as pl
from jax.experimental.pallas import tpu as pltpu
from jax.sharding import PartitionSpec as P

BF = jnp.bfloat16
F32 = jnp.float32
OWN, PREV, NEXT, FAR = 0, 1, 2, 3


def gelu_value(pre):
    phi = 0.5 * (1.0 + lax.erf(pre * 0.7071067811865476))
    return pre * phi


def gelu_slope(pre):
    phi = 0.5 * (1.0 + lax.erf(pre * 0.7071067811865476))
    return phi + pre * jnp.exp(-0.5 * pre * pre) * 0.3989422804014327


def dot(left, right, left_dim, right_dim):
    return lax.dot_general(
        left, right, (((left_dim,), (right_dim,)), ((), ())), preferred_element_type=F32
    )


class Wire:
    def __init__(self, send_sems, recv_sems):
        self.send_sems, self.recv_sems = send_sems, recv_sems
        self.count = 0
        self.turn = 0
        self.last = {}

    def slot(self):
        self.count += 1
        return self.count - 1

    def copy(self, src, dst, device, slot):
        turn = self.turn % N_SENDS
        self.turn += 1
        made = pltpu.make_async_remote_copy(
            src_ref=src,
            dst_ref=dst,
            send_sem=self.send_sems.at[turn],
            recv_sem=self.recv_sems.at[slot],
            device_id=device,
            device_id_type=pl.DeviceIdType.MESH,
        )
        self.finish(turn)
        return made, turn

    def finish(self, turn):
        if turn in self.last:
            made, when = self.last.pop(turn)
            if when is None:
                made.wait_send()
            else:
                pl.when(when)(made.wait_send)

    def started(self, pair, when=None):
        self.last[pair[1]] = (pair[0], when)

    def send(self, src, dst, device, slot=None, when=None):
        pair = self.copy(src, dst, device, self.slot() if slot is None else slot)
        if when is None:
            pair[0].start()
        else:
            pl.when(when)(pair[0].start)
        self.started(pair, when)
        return pair[0]

    def wait_for(self, ref, slot):
        pltpu.make_async_copy(ref, ref, self.recv_sems.at[slot]).wait()

    def drain(self):
        for turn in list(self.last):
            self.finish(turn)


class RingSum:
    def __init__(self, wire, plus, minus, block, half, bufs):
        self.w, self.plus, self.minus, self.block, self.half = wire, plus, minus, block, half
        self.r1a, self.r1b, self.r2p, self.r2m, self.ga, self.gb = bufs

    def start(self):
        self.start_far()
        self.start_near()

    def start_far(self):
        w = self.w
        self.c1 = w.send(self.block(2, 0), self.r1a, self.plus)
        self.c2 = w.send(self.block(2, 1), self.r1b, self.minus)

    def start_near(self):
        w, half = self.w, self.half
        self.sp, self.sm = w.slot(), w.slot()
        w.send(self.block(1, 1), half(self.r2p, 1), self.plus, self.sp)
        w.send(self.block(-1, 0), half(self.r2m, 0), self.minus, self.sm)

    def mid(self):
        w, half = self.w, self.half
        self.c1.wait_recv()
        self.ga[...] = (self.block(1, 0)[...].astype(F32) + self.r1a[...].astype(F32)).astype(BF)
        w.send(self.ga, half(self.r2p, 0), self.plus, self.sp)
        self.c2.wait_recv()
        self.gb[...] = (self.block(-1, 1)[...].astype(F32) + self.r1b[...].astype(F32)).astype(BF)
        w.send(self.gb, half(self.r2m, 1), self.minus, self.sm)

    def end(self, own):
        self.w.wait_for(self.r2p, self.sp)
        self.w.wait_for(self.r2m, self.sm)
        return own + self.r2p[...].astype(F32) + self.r2m[...].astype(F32)


class RingCopy:
    def __init__(self, wire, plus, minus, own, at_plus, at_minus, near, far):
        self.w, self.plus, self.minus = wire, plus, minus
        self.own, self.at_plus, self.at_minus, self.near, self.far = own, at_plus, at_minus, near, far

    def start(self):
        w = self.w
        self.p0 = w.send(self.own(0), self.at_plus(0), self.plus)
        self.m1 = w.send(self.own(1), self.at_minus(1), self.minus)
        self.p1 = w.send(self.own(1), self.at_plus(1), self.plus)
        self.m0 = w.send(self.own(0), self.at_minus(0), self.minus)

    def mid(self):
        w = self.w
        self.p0.wait_recv()
        self.f0 = w.send(self.near(-1, 0), self.far(-1, 0), self.plus)
        self.m1.wait_recv()
        self.f1 = w.send(self.near(1, 1), self.far(1, 1), self.minus)

    def near_end(self):
        self.p1.wait_recv()
        self.m0.wait_recv()

    def far_end(self):
        self.f0.wait_recv()
        self.f1.wait_recv()


class BlockCopy:
    def __init__(self, wire, plus, minus, view, whole):
        self.w, self.plus, self.minus, self.view, self.whole = wire, plus, minus, view, whole

    def start(self):
        w, mine = self.w, self.whole(0)
        self.p = w.send(mine, mine, self.plus)
        self.m = w.send(mine, mine, self.minus)
        self.slot = w.slot()

    def mid(self):
        w = self.w
        self.p.wait_recv()
        half = self.view(-1, 0)
        w.send(half, half, self.plus, self.slot)
        self.m.wait_recv()
        half = self.view(1, 1)
        w.send(half, half, self.minus, self.slot)

    def end(self):
        self.w.wait_for(self.whole(2), self.slot)


SCRATCH = dict(
    x=((512, 1024), BF),
    c=((512, 1024), BF),
    tk=((256, 1024), BF),
    wu=((4, 1024, 128), BF),
    wd=((512, 1024), BF),
    sstat=((8, 256), F32),
    rstat=((3, 8, 256), F32),
    mean=((256, 128), F32),
    rstd=((256, 128), F32),
    part=((2, 4, 512, 128), BF),
    pa=((2, 4, 256, 128), BF),
    pb=((2, 4, 256, 128), BF),
    pf=((2, 4, 256, 128), BF),
    pg=((2, 4, 256, 128), BF),
    pre=((4, 256, 128), F32),
    hid=((2, 4, 512, 128), BF),
    bs=((2, 256, 1024), BF),
    br=((2, 256, 1024), BF),
    xacc=((2, 256, 1024), F32),
    xown=((2, 4, 16, 1024), F32),
    xs=((2, 4, 4, 16, 1024), BF),
    x1a=((2, 4, 16, 512), BF),
    x1b=((2, 4, 16, 512), BF),
    x2p=((2, 4, 16, 1024), BF),
    x2m=((2, 4, 16, 1024), BF),
    xga=((2, 4, 16, 512), BF),
    xgb=((2, 4, 16, 512), BF),
    zs=((2, 4, 16, 1024), BF),
    z1a=((2, 16, 512), BF),
    z1b=((2, 16, 512), BF),
    z2p=((2, 16, 1024), BF),
    z2m=((2, 16, 1024), BF),
    zga=((2, 16, 512), BF),
    zgb=((2, 16, 512), BF),
    fin=((2, 256, 1024), BF),
    ts=((1, 128), F32),
    tr=((3, 1, 128), F32),
    tz=((4, 1, 128), F32),
    gdp=((512, 1024), BF),
    gdo=((128, 1024), F32),
    gd1a=((64, 1024), BF),
    gd1b=((64, 1024), BF),
    gd2p=((128, 1024), BF),
    gd2m=((128, 1024), BF),
    gdga=((64, 1024), BF),
    gdgb=((64, 1024), BF),
    gdout=((128, 1024), BF),
    gup=((4, 1024, 128), BF),
    guo=((1024, 128), F32),
    gu1a=((512, 128), BF),
    gu1b=((512, 128), BF),
    gu2p=((1024, 128), BF),
    gu2m=((1024, 128), BF),
    guga=((512, 128), BF),
    gugb=((512, 128), BF),
    guout=((1024, 128), BF),
)
N_SEMS = 149
N_SENDS = 32


def rows_of(index, size):
    return pl.ds(pl.multiple_of(index * size, size), size)


def kernel(tok_h, wu_h, wd_h, cot_h, mix_h, ing_h, gu_h, gd_h, *scratch):
    s = dict(zip(SCRATCH, scratch))
    send_sems, recv_sems, local_sems = scratch[len(SCRATCH) :]
    wire = Wire(send_sems, recv_sems)

    fsdp, trow, tcol = lax.axis_index("fsdp"), lax.axis_index("trow"), lax.axis_index("tcol")
    y, core = fsdp // 2, lax.rem(fsdp, 2)
    xx, zh = trow // 4, lax.rem(trow, 4)
    zl = tcol

    def at(dy=0, dcore=0, dx=0, dzh=0):
        return (
            lax.rem(y + dy, 4) * 2 + lax.rem(core + dcore, 2),
            lax.rem(xx + dx, 4) * 4 + lax.rem(zh + dzh, 4),
            tcol,
        )

    def at_zl(index):
        return (fsdp, trow, index)

    partner = at(dcore=1)
    y_plus, y_minus = at(dy=1), at(dy=3)
    x_plus, x_minus = at(dx=1), at(dx=3)
    right = zl // 2
    mate = zl + 1 - 2 * lax.rem(zl, 2)
    far_hub = 2 - right
    far_end = 3 - 3 * right
    is_hub = jnp.logical_or(zl == 1, zl == 2)
    is_end = jnp.logical_or(zl == 0, zl == 3)

    barrier = pltpu.get_barrier_semaphore()
    z_plus, z_minus = at(dzh=1), at(dzh=3)
    others = [partner, y_plus, y_minus, x_plus, x_minus, z_plus, z_minus]
    others += [at_zl(lax.rem(zl + k, 4)) for k in (1, 2, 3)]
    loads = [
        pltpu.make_async_copy(src, dst, local_sems.at[i])
        for i, (src, dst) in enumerate(
            (
                (tok_h, s["tk"]),
                (wu_h, s["wu"].at[0]),
                (wd_h, s["wd"].at[0:128]),
                (cot_h, s["c"].at[0:256]),
            )
        )
    ]
    for load in loads:
        load.start()
    for other in others:
        pl.semaphore_signal(
            barrier, inc=1, device_id=other, device_id_type=pl.DeviceIdType.MESH
        )

    loads[0].wait()
    tok = s["tk"][...].astype(F32)
    sum_one = jnp.sum(tok, axis=1, keepdims=True)
    sum_two = jnp.sum(tok * tok, axis=1, keepdims=True)
    lane = lax.broadcasted_iota(jnp.int32, (256, 128), 1)
    both = jnp.where(lane == 0, sum_one, jnp.where(lane == 1, sum_two, 0.0))
    s["sstat"][...] = jnp.transpose(both)[0:8]
    for load in loads[1:]:
        load.wait()
    pl.semaphore_wait(barrier, len(others))

    def wu_at(pos, h):
        return s["wu"].at[pos, h * 512 : (h + 1) * 512]

    def wd_at(pos, h):
        return s["wd"].at[pos * 128 + h * 64 : pos * 128 + (h + 1) * 64]

    def weights(view):
        return RingCopy(
            wire,
            y_plus,
            y_minus,
            own=lambda h: view(OWN, h),
            at_plus=lambda h: view(PREV, h),
            at_minus=lambda h: view(NEXT, h),
            near=lambda rel, h: view(PREV if rel < 0 else NEXT, h),
            far=lambda rel, h: view(FAR, h),
        )

    ups, downs = weights(wu_at), weights(wd_at)
    ups.start()
    stat_slot = wire.slot()
    for k in (1, 2, 3):
        wire.send(s["sstat"], s["rstat"].at[k - 1], at_zl(lax.rem(zl + k, 4)), stat_slot)
    cot_copy = wire.send(s["c"].at[0:256], s["c"].at[256:512], partner)

    class Exchange:
        def __init__(self, which, pos, first, count):
            self.which, self.first, self.count = which, first, count
            self.pos = pos
            self.i = (which, pos, slice(first, first + count))
            self.slots = [wire.slot() for _ in range(6)]

        def rows(self, side):
            if isinstance(side, int):
                return pl.ds(side * 256 + self.first, self.count)
            return pl.ds(pl.multiple_of(side * 256 + self.first, 128), self.count)

        def part(self, side):
            return s["part"].at[self.which, self.pos, self.rows(side)]

        def back(self, side):
            return s["hid"].at[self.which, self.pos, self.rows(side)]

        def start(self):
            self.far = wire.send(
                self.part(1 - right), s["pb"].at[self.i], at_zl(mate), self.slots[0], is_end
            )

        def start_side(self, side):
            to, part, (far, near) = at_zl(mate), self.part(side), self.slots[0:2]
            self.near = wire.send(part, s["pa"].at[self.i], to, near, zl == 3 * side)
            self.far = wire.send(part, s["pb"].at[self.i], to, far, zl == 3 - 3 * side)

        def start_near(self):
            self.near = wire.send(
                self.part(right), s["pa"].at[self.i], at_zl(mate), self.slots[1], is_end
            )

        def mid(self):
            pair = wire.copy(s["pg"].at[self.i], s["pf"].at[self.i], at_zl(far_hub), self.slots[2])

            @pl.when(is_hub)
            def _():
                self.far.wait_recv()
                both = self.part(1 - right)[...].astype(F32) + s["pb"][self.i].astype(F32)
                s["pg"][self.i] = both.astype(BF)
                pair[0].start()

            wire.started(pair, is_hub)
            self.cross = pair[0]

        def end(self, finish):
            mine = self.back(right)
            across = wire.copy(mine, mine, at_zl(far_hub), self.slots[3])
            down = wire.copy(mine, mine, at_zl(mate), self.slots[4])

            @pl.when(is_hub)
            def _():
                self.near.wait_recv()
                self.cross.wait_recv()
                total = self.part(right)[...].astype(F32) + s["pa"][self.i].astype(F32)
                total = total + s["pf"][self.i].astype(F32)
                s["hid"][self.which, self.pos, self.rows(right)] = finish(total, self.i)
                across[0].start()
                down[0].start()

            wire.started(across, is_hub)
            wire.started(down, is_hub)
            self.across, self.down = across[0], down[0]

        def back_mid(self):
            theirs = self.back(1 - right)
            pair = wire.copy(theirs, theirs, at_zl(mate), self.slots[5])

            @pl.when(is_hub)
            def _():
                self.across.wait_recv()
                pair[0].start()

            wire.started(pair, is_hub)
            self.passed = pair[0]

        def back_end(self):
            @pl.when(is_end)
            def _():
                self.down.wait_recv()
                self.passed.wait_recv()

    class LastExchange(Exchange):
        def end(self, finish):
            mine = self.back(right)
            beyond = wire.copy(mine, mine, at_zl(far_end), self.slots[5])
            across = wire.copy(mine, mine, at_zl(far_hub), self.slots[3])
            down = wire.copy(mine, mine, at_zl(mate), self.slots[4])

            @pl.when(is_hub)
            def _():
                self.near.wait_recv()
                self.cross.wait_recv()
                total = self.part(right)[...].astype(F32) + s["pa"][self.i].astype(F32)
                total = total + s["pf"][self.i].astype(F32)
                s["hid"][self.which, self.pos, self.rows(right)] = finish(total, self.i)
                beyond[0].start()
                across[0].start()
                down[0].start()

            for pair in (beyond, across, down):
                wire.started(pair, is_hub)
            self.passed, self.across, self.down = beyond[0], across[0], down[0]

        def back_mid(self):
            pl.when(is_hub)(self.across.wait_recv)

    def gelu_of(total, i):
        s["pre"][i[1:]] = total
        return gelu_value(total).astype(BF)

    def dpre_of(total, i):
        return (total * gelu_slope(s["pre"][i[1:]])).astype(BF)

    pres = [[Exchange(0, pos, 0, 256)] for pos in range(4)]
    dhs = [[Exchange(1, pos, 0, 256)] for pos in range(3)]
    dhs.append([LastExchange(1, 3, 0, 128), LastExchange(1, 3, 128, 128)])

    def every(exchanges, step, *args):
        for e in exchanges:
            getattr(e, step)(*args)

    def side_by_side(blocks):
        return blocks[0] if len(blocks) == 1 else jnp.concatenate(blocks, axis=1)

    def put_part(which, first, last, value):
        for pos in range(first, last):
            lanes = slice((pos - first) * 128, (pos - first + 1) * 128)
            s["part"][which, pos] = value[:, lanes].astype(BF)

    def pre_part(first, last):
        blocks = side_by_side([s["wu"][pos] for pos in range(first, last)])
        put_part(0, first, last, dot(s["x"][...], blocks, 1, 0))
        for step in ("start", "start_near"):
            for pos in range(first, last):
                every(pres[pos], step)

    def dh_part(first, last):
        lanes = slice(first * 128, last * 128)
        put_part(1, first, last, dot(s["c"][...], s["wd"][lanes], 1, 1))
        for step in ("start", "start_near"):
            for pos in range(first, last):
                every(dhs[pos], step)

    def pre_done(pos):
        every(pres[pos], "end", gelu_of)

    def dh_done(pos):
        every(dhs[pos], "end", dpre_of)

    def own_block(which, side, value):
        s["part"][which, 0, side * 256 : (side + 1) * 256] = value.astype(BF)
        every((pres, dhs)[which][0], "start_side", side)

    own_block(1, 0, dot(s["c"][0:256], s["wd"][0:128], 1, 1))
    cot_copy.wait_recv()
    own_block(1, 1, dot(s["c"][256:512], s["wd"][0:128], 1, 1))

    wire.wait_for(s["rstat"], stat_slot)
    total = s["sstat"][...] + s["rstat"][0] + s["rstat"][1] + s["rstat"][2]
    total = jnp.transpose(jnp.concatenate([total, jnp.zeros((120, 256), F32)], axis=0))
    mean = total[:, 0:1] / 4096.0
    var = total[:, 1:2] / 4096.0 - mean * mean
    rstd = lax.rsqrt(var + 1e-05)
    s["mean"][...] = jnp.broadcast_to(mean, (256, 128))
    s["rstd"][...] = jnp.broadcast_to(rstd, (256, 128))
    s["x"][0:256] = ((s["tk"][...].astype(F32) - mean) * rstd).astype(BF)
    x_copy = wire.send(s["x"].at[0:256], s["x"].at[256:512], partner)
    own_block(0, 0, dot(s["x"][0:256], s["wu"][0], 1, 0))
    ups.mid()
    downs.start()
    x_copy.wait_recv()
    own_block(0, 1, dot(s["x"][256:512], s["wu"][0], 1, 0))
    every(dhs[0], "mid")
    ups.near_end()
    pre_part(1, 3)
    every(pres[0], "mid")
    ups.far_end()
    pre_part(3, 4)
    pre_done(0)
    dh_done(0)
    every(pres[1], "mid")
    every(pres[2], "mid")
    downs.mid()
    every(pres[3], "mid")
    every(pres[0], "back_mid")
    every(dhs[0], "back_mid")
    downs.near_end()
    dh_part(1, 3)
    pre_done(1)
    pre_done(2)
    every(dhs[1], "mid")
    downs.far_end()
    dh_part(3, 4)
    every(dhs[2], "mid")
    pre_done(3)
    every(pres[1], "back_mid")
    every(pres[2], "back_mid")
    dh_done(1)
    every(pres[3], "back_mid")
    every(dhs[3], "mid")
    dh_done(2)
    every(dhs[1], "back_mid")

    def rows(rel_x, rel_z):
        first = lax.rem(xx + rel_x, 4) * 64 + lax.rem(zh + rel_z, 4) * 16
        return pl.ds(pl.multiple_of(first, 16), 16)

    mine = rows(0, 0)
    steps = (2, 1, 3, 0)
    chunks = (slice(0, 1), slice(1, 4))

    def out_part(o, product):
        s["bs"][o] = product(1).astype(BF)
        sent = []
        for rel in (2, 1, 3, 0):
            r = rows_of(lax.rem(xx + rel, 4), 64)
            sent.append(wire.send(s["bs"].at[o, r], s["br"].at[o, r], partner))
        s["xacc"][o] = product(0)
        return sent

    def over_x(o, k):
        which = pl.ds(chunks[k].start, chunks[k].stop - chunks[k].start)

        def block(rel, h):
            return s["xs"].at[o, which, rel % 4, :, h * 512 : (h + 1) * 512]

        def half(ref, h):
            return ref.at[:, :, h * 512 : (h + 1) * 512]

        names = ("x1a", "x1b", "x2p", "x2m", "xga", "xgb")
        return RingSum(wire, x_plus, x_minus, block, half, [s[n].at[o, which] for n in names])

    x_sums = [[over_x(o, k) for k in (0, 1)] for o in (0, 1)]

    def x_start(o, copies):
        for rel, copy in zip((2, 1, 3, 0), copies):
            copy.wait_recv()
            for k, chunk in enumerate(chunks):
                for i in range(chunk.start, chunk.stop):
                    r = rows(rel, steps[i])
                    value = s["xacc"][o, r] + s["br"][o, r].astype(F32)
                    if rel == 0:
                        s["xown"][o, i] = value
                    else:
                        s["xs"][o, i, rel] = value.astype(BF)
                if rel == 2:
                    x_sums[o][k].start_far()
            if rel == 3:
                x_sums[o][0].start_near()
                x_sums[o][1].start_near()

    def over_z(o):
        def block(rel, h):
            return s["zs"].at[o, rel % 4, :, h * 512 : (h + 1) * 512]

        def half(ref, h):
            return ref.at[:, h * 512 : (h + 1) * 512]

        names = ("z1a", "z1b", "z2p", "z2m", "zga", "zgb")
        return RingSum(wire, at(dzh=1), at(dzh=3), block, half, [s[n].at[o] for n in names])

    z_sums = [over_z(0), over_z(1)]

    def z_start(o, k):
        chunk = chunks[k]
        value = x_sums[o][k].end(s["xown"][o, chunk])
        s["xown"][o, chunk] = value
        for i in range(chunk.start, min(chunk.stop, 3)):
            s["zs"][o, steps[i]] = value[i - chunk.start].astype(BF)
        if k == 0:
            z_sums[o].start_far()
        else:
            z_sums[o].start_near()

    def z_done(o):
        return z_sums[o].end(s["xown"][o, 3])

    def back_z(o):
        def view(rel, h):
            return s["fin"].at[o, rows(0, rel % 4), h * 512 : (h + 1) * 512]

        spread = RingCopy(
            wire,
            at(dzh=1),
            at(dzh=3),
            own=lambda h: view(0, h),
            at_plus=lambda h: view(0, h),
            at_minus=lambda h: view(0, h),
            near=view,
            far=view,
        )
        spread.start()
        return spread

    def back_x(o, rel_z):
        def view(rel, h):
            return s["fin"].at[o, rows(rel % 4, rel_z % 4), h * 512 : (h + 1) * 512]

        def whole(rel):
            return s["fin"].at[o, rows(rel % 4, rel_z % 4)]

        return BlockCopy(wire, x_plus, x_minus, view, whole)

    def back_x_start(o, rel_z):
        spread = back_x(o, rel_z)
        spread.start()
        return spread

    pos_of = {1: NEXT, 2: FAR, -1: PREV}

    def gd_block(rel, h):
        first = pos_of[rel] * 128 + h * 64
        return s["gdp"].at[first : first + 64]

    def gu_block(rel, h):
        pos = pos_of[rel]
        return s["gup"].at[pos, h * 512 : (h + 1) * 512]

    gd_names = ("gd1a", "gd1b", "gd2p", "gd2m", "gdga", "gdgb")
    gu_names = ("gu1a", "gu1b", "gu2p", "gu2m", "guga", "gugb")
    gd_sum = RingSum(
        wire, y_plus, y_minus, gd_block, lambda r, h: r.at[h * 64 : (h + 1) * 64],
        [s[n] for n in gd_names],
    )
    gu_sum = RingSum(
        wire, y_plus, y_minus, gu_block, lambda r, h: r.at[h * 512 : (h + 1) * 512],
        [s[n] for n in gu_names],
    )

    def hid(which, first, last):
        return side_by_side([s["hid"][which, pos, first:last] for pos in range(4)])

    for pos in range(4):
        every(pres[pos], "back_end")
    branch_copy = out_part(
        0, lambda half: dot(hid(0, half * 256, half * 256 + 256), s["wd"][...], 1, 0)
    )
    dh_done(3)
    every(dhs[2], "back_mid")
    x_start(0, branch_copy)
    grad = dot(hid(0, 0, 512), s["c"][...], 0, 0)
    s["gdo"][...] = grad[0:128]
    s["gdp"][128:512] = grad[128:512].astype(BF)
    gd_sum.start()
    every(dhs[3], "back_mid")
    for pos in range(4):
        every(dhs[pos], "back_end")

    dnorm_copy = out_part(
        1,
        lambda half: dot(
            hid(1, half * 256, half * 256 + 256),
            side_by_side([s["wu"][pos] for pos in range(4)]),
            1,
            1,
        ),
    )
    x_sums[0][0].mid()
    x_sums[0][1].mid()
    x_start(1, dnorm_copy)
    grad = dot(s["x"][...], hid(1, 0, 512), 0, 0)
    s["guo"][...] = grad[:, 0:128]
    for pos in (1, 2, 3):
        s["gup"][pos] = grad[:, pos * 128 : (pos + 1) * 128].astype(BF)
    gu_sum.start()
    z_start(0, 0)
    z_start(0, 1)
    x_sums[1][0].mid()
    x_sums[1][1].mid()
    gd_sum.mid()
    z_start(1, 0)
    z_start(1, 1)

    z_sums[0].mid()

    lane = lax.broadcasted_iota(jnp.int32, (16, 128), 1)
    row = lax.broadcasted_iota(jnp.int32, (16, 128), 0)
    line = jnp.zeros((1, 128), F32)
    for i in range(4):
        part = s["xown"][1, i]
        r = rows(0, steps[i])
        xhat = (s["tk"][r, :].astype(F32) - s["mean"][r, 0:1]) * s["rstd"][r, 0:1]
        first = jnp.sum(part, axis=1, keepdims=True)
        second = jnp.sum(part * xhat, axis=1, keepdims=True)
        place = row + lax.rem(zh + steps[i], 4) * 16
        spot = jnp.where(lane == place, first, jnp.where(lane == place + 64, second, 0.0))
        line = line + jnp.sum(spot, axis=0, keepdims=True)
    s["ts"][...] = line
    moment_slot = wire.slot()
    for k in (1, 2, 3):
        wire.send(s["ts"], s["tr"].at[k - 1], at_zl(lax.rem(zl + k, 4)), moment_slot)
    gu_sum.mid()
    wire.wait_for(s["tr"], moment_slot)
    s["tz"][0] = s["ts"][...] + s["tr"][0] + s["tr"][1] + s["tr"][2]
    moment_copies = [
        wire.send(s["tz"].at[0], s["tz"].at[d], at(dzh=d)) for d in (2, 1, 3)
    ]
    z_sums[1].mid()
    s["fin"][0, mine, :] = (s["tk"][mine, :].astype(F32) + z_done(0)).astype(BF)
    z_back0 = back_z(0)
    x_backs0 = [back_x_start(0, 0)]
    s["gdout"][...] = gd_sum.end(s["gdo"][...]).astype(BF)
    gd_out = pltpu.make_async_copy(s["gdout"], gd_h, local_sems.at[4])
    gd_out.start()

    dnorm = z_done(1)
    for c in moment_copies:
        c.wait_recv()
    line = s["tz"][0] + s["tz"][1] + s["tz"][2] + s["tz"][3]
    place = row + zh * 16
    moment_one = jnp.sum(jnp.where(lane == place, line, 0.0), axis=1, keepdims=True) / 4096.0
    moment_two = jnp.sum(jnp.where(lane == place + 64, line, 0.0), axis=1, keepdims=True) / 4096.0
    rstd = s["rstd"][mine, 0:1]
    xhat = (s["tk"][mine, :].astype(F32) - s["mean"][mine, 0:1]) * rstd
    grad = s["c"][mine, :].astype(F32) + rstd * (dnorm - moment_one - xhat * moment_two)
    s["fin"][1, mine, :] = grad.astype(BF)
    z_back1 = back_z(1)
    x_backs1 = [back_x_start(1, 0)]
    x_backs0[0].mid()
    z_back0.mid()
    z_back0.near_end()
    x_backs0 += [back_x_start(0, 1), back_x_start(0, 3)]
    x_backs1[0].mid()
    x_backs0[1].mid()
    x_backs0[2].mid()
    z_back0.far_end()
    x_backs0.append(back_x_start(0, 2))
    z_back1.mid()
    z_back1.near_end()
    x_backs1 += [back_x_start(1, 1), back_x_start(1, 3)]
    s["guout"][...] = gu_sum.end(s["guo"][...]).astype(BF)
    gu_out = pltpu.make_async_copy(s["guout"], gu_h, local_sems.at[5])
    gu_out.start()
    x_backs1[1].mid()
    x_backs1[2].mid()
    x_backs0[3].mid()
    z_back1.far_end()
    x_backs1.append(back_x_start(1, 2))
    for spread in x_backs0:
        spread.end()
    mix_out = pltpu.make_async_copy(s["fin"].at[0], mix_h, local_sems.at[6])
    mix_out.start()
    x_backs1[3].mid()
    for spread in x_backs1:
        spread.end()
    ing_out = pltpu.make_async_copy(s["fin"].at[1], ing_h, local_sems.at[7])
    ing_out.start()
    wire.drain()
    assert wire.count == N_SEMS, wire.count
    for out in (gd_out, gu_out, mix_out, ing_out):
        out.wait()


def hand_over(*refs):
    sems = refs[-1]
    copies = [pltpu.make_async_copy(refs[i], refs[4 + i], sems.at[i]) for i in range(4)]
    for c in copies:
        c.start()
    for c in copies:
        c.wait()


def local(tokens, w_up, w_down, cotangent):
    scratch = [pltpu.VMEM(shape, dtype) for shape, dtype in SCRATCH.values()]
    scratch += [pltpu.SemaphoreType.DMA((N_SENDS,)), pltpu.SemaphoreType.DMA((N_SEMS,))]
    scratch += [pltpu.SemaphoreType.DMA((8,))]
    outs = (
        jax.ShapeDtypeStruct(tokens.shape, BF),
        jax.ShapeDtypeStruct(cotangent.shape, BF),
        jax.ShapeDtypeStruct(w_up.shape, BF),
        jax.ShapeDtypeStruct(w_down.shape, BF),
    )
    tokens, w_up, w_down, cotangent = (
        pltpu.with_memory_space_constraint(a, pltpu.HBM)
        for a in (tokens, w_up, w_down, cotangent)
    )
    made = pl.pallas_call(
        kernel,
        out_shape=outs,
        in_specs=[pl.BlockSpec(memory_space=pltpu.HBM)] * 4,
        out_specs=[pl.BlockSpec(memory_space=pl.ANY)] * 4,
        scratch_shapes=scratch,
        compiler_params=pltpu.CompilerParams(
            collective_id=0, has_side_effects=True, vmem_limit_bytes=32 * 1024 * 1024
        ),
        name="block",
    )(tokens, w_up, w_down, cotangent)
    return pl.pallas_call(
        hand_over,
        out_shape=outs,
        in_specs=[pl.BlockSpec(memory_space=pl.ANY)] * 4,
        out_specs=[pl.BlockSpec(memory_space=pl.ANY)] * 4,
        scratch_shapes=[pltpu.SemaphoreType.DMA((4,))],
        compiler_params=pltpu.CompilerParams(vmem_limit_bytes=1024 * 1024),
        name="hand_over",
    )(*made)


def solution(mesh):
    return jax.shard_map(
        local,
        mesh=mesh,
        in_specs=(
            P("fsdp", "tcol"),
            P("tcol", ("fsdp", "trow")),
            P(("fsdp", "trow"), "tcol"),
            P("fsdp", "tcol"),
        ),
        out_specs=(
            P("fsdp", "tcol"),
            P("fsdp", "tcol"),
            P("tcol", ("fsdp", "trow")),
            P(("fsdp", "trow"), "tcol"),
        ),
        check_vma=False,
    )
```
